256 devices in a mesh: img: 32 (over z, x), row: 8 (over y, core).
Axes of the slice: x: 4, y: 4, z: 8, core: 2. Of those that a mesh axis runs over, the one named last changes fastest.
Arguments:
- tokens: bfloat16 [32, 64, 128, 1024], P('img', 'row'), may hold values from -14 to 14
- proj_weight: bfloat16 [1024, 256], replicated, may hold values from -0.1875 to 0.1875
- proj_bias: float32 [256], replicated, may hold values from -3 to 3
- conv_weight: bfloat16 [4, 3, 3, 256, 256], replicated, may hold values from -0.125 to 0.125
- bn_gain: float32 [4, 256], replicated, may hold values from 0.1 to 1.9
- bn_bias: float32 [4, 256], replicated, may hold values from -3 to 3
Outputs:
- joining_out: bfloat16 [32, 64, 128, 256], P('img', 'row')
The draws below stay inside these ranges and needn't reach their ends.
All inputs are finite; a program needn't handle non-finite values.
Results may differ from the reference program's by a relative error of at most 0.0071.
Values may be sent and summed in bfloat16 or wider, within the bound.
No kernel may reach another device: no remote copies, remote signals or barrier semaphores. Data moves between devices by JAX's collectives and lax.ppermute only.
A program may use at most 64 MiB of HBM per device.

```python
import math
import jax
import jax.numpy as jnp
from jax import lax

EMBED = 1024
FW = 256
COLS = 128
IMAGES = 32
HEIGHT = 64


def draw_tokens(key, part):
    key_image, key_row, key_base = jax.random.split(key, 3)
    image_scale = jnp.exp(jax.random.uniform(key_image, (IMAGES, 1, 1, 1), jnp.float32, 0.0, math.log(4.0)))
    row_scale = jnp.exp(jax.random.uniform(key_row, (1, HEIGHT, 1, 1), jnp.float32, 0.0, math.log(2.5)))
    base = jnp.clip(jax.random.normal(key_base, (IMAGES, HEIGHT, COLS, EMBED), jnp.float32), -4.0, 4.0)
    return (base * image_scale * row_scale / 3.0).astype(jnp.bfloat16)


def centred(key, dims, deviation, most, kind=jnp.bfloat16):
    return jnp.clip(deviation * jax.random.normal(key, dims, jnp.float32), -most, most).astype(kind)


def setup_inputs(seed: int = 0) -> dict:
    key_of = jax.random.split(jax.random.key(seed), 7)
    tokens = draw_tokens(jax.random.fold_in(key_of[6], 71), 0)
    proj_weight = centred(key_of[1], (EMBED, FW), EMBED ** -0.5, 0.1875)
    proj_bias = centred(key_of[2], (FW,), 0.5, 3.0, jnp.float32)
    conv_weight = centred(key_of[3], (4, 3, 3, FW, FW), (9 * FW) ** -0.5, 0.125)
    bn_gain = jnp.clip(1.0 + 0.18 * jax.random.normal(key_of[4], (4, FW), jnp.float32), 0.1, 1.9)
    bn_bias = centred(key_of[5], (4, FW), 0.5, 3.0, jnp.float32)
    return {"tokens": tokens, "proj_weight": proj_weight, "proj_bias": proj_bias, "conv_weight": conv_weight, "bn_gain": bn_gain, "bn_bias": bn_bias}


epsilon = 1e-05

def conv_three(source, kernel):
    return lax.conv_general_dilated(source.astype(jnp.float32), kernel.astype(jnp.float32), (1, 1), ((1, 1), (1, 1)), dimension_numbers=('NHWC', 'HWIO', 'NHWC'), precision=lax.Precision.HIGHEST)

def batch_norm(conv_out, gain_row, shift_row):
    average = lax.optimization_barrier(jnp.mean(conv_out, axis=(0, 1, 2)))
    spread = lax.optimization_barrier(jnp.mean(jnp.square(conv_out - average), axis=(0, 1, 2)))
    return (conv_out - average) * lax.rsqrt(spread + epsilon) * gain_row + shift_row

def residual_unit(source, conv_weight, bn_gain, bn_bias, first):
    active = jax.nn.relu(source)
    conv_first = conv_three(active, conv_weight[first])
    hidden = jax.nn.relu(batch_norm(conv_first, bn_gain[first], bn_bias[first])).astype(jnp.bfloat16)
    conv_second = conv_three(hidden, conv_weight[first + 1])
    return source.astype(jnp.float32) + batch_norm(conv_second, bn_gain[first + 1], bn_bias[first + 1])

def reference(tokens, proj_weight, proj_bias, conv_weight, bn_gain, bn_bias):
    img_count, row_count, col_count, embed_dim = tokens.shape
    flat = jnp.dot(tokens.reshape(-1, embed_dim), proj_weight, preferred_element_type=jnp.float32) + proj_bias
    feature = flat.astype(jnp.bfloat16).reshape(img_count, row_count, col_count, -1)
    joined = residual_unit(feature, conv_weight, bn_gain, bn_bias, 0).astype(jnp.bfloat16)
    return residual_unit(joined, conv_weight, bn_gain, bn_bias, 2).astype(jnp.bfloat16)
```

```python
import functools

import jax
import jax.numpy as jnp
from jax import lax
from jax.experimental import pallas as pl
from jax.experimental.pallas import tpu as pltpu
from jax.sharding import PartitionSpec as P

EPS = 1e-05
HALO = 4
STEP = 4
AHEAD = 0
VM = pl.BlockSpec(memory_space=pltpu.VMEM)
HBM = pl.BlockSpec(memory_space=pltpu.HBM)
BF = jnp.bfloat16
F32 = jnp.float32
PARAMS = pltpu.CompilerParams(vmem_limit_bytes=24 << 20)


def sds(shape, dtype):
    return jax.ShapeDtypeStruct(shape, dtype)


def in_hbm(x):
    return pltpu.with_memory_space_constraint(x, pltpu.HBM)


def in_vmem(x):
    return pltpu.with_memory_space_constraint(x, pltpu.VMEM)


def put_row(a3, row, x):
    cols, ch = x.shape
    col = lax.broadcasted_iota(jnp.int32, x.shape, 0)
    a3[row, :, ch : 2 * ch] = x.astype(BF)
    a3[row, :, 0:ch] = jnp.where(col == 0, 0.0, pltpu.roll(x, 1, 0)).astype(BF)
    a3[row, :, 2 * ch :] = jnp.where(col == cols - 1, 0.0, pltpu.roll(x, cols - 1, 0)).astype(BF)


def conv_block(a3, wbuf, first, rows):
    cols, k = a3.shape[1:]
    acc = None
    for dy in range(3):
        lhs = a3[first + dy : first + dy + rows].reshape(rows * cols, k)
        part = jnp.dot(lhs, wbuf[dy].reshape(k, -1), preferred_element_type=F32)
        acc = part if acc is None else acc + part
    return acc


def fold8(x):
    return x.reshape(-1, 8, x.shape[-1]).sum(axis=0)


def norm_terms(stats_ref, gain_ref, bias_ref, k, total):
    s = jnp.sum(stats_ref[...], axis=0)
    ch = s.shape[-1] // 2
    mean = s[:, :ch] / total
    spread = jnp.maximum(s[:, ch:] / total - mean * mean, 0.0)
    return mean, lax.rsqrt(spread + EPS) * gain_ref[k : k + 1, :], bias_ref[k : k + 1, :]


def write_stats(out_ref, sums, squares):
    both = jnp.concatenate(
        [jnp.sum(sums, axis=0, keepdims=True), jnp.sum(squares, axis=0, keepdims=True)], axis=1
    )
    out_ref[...] = jnp.broadcast_to(both[None], out_ref.shape)


def inside(local_row, strip, axis):
    if 0 <= local_row < strip:
        return None
    r = lax.axis_index(axis)
    edge = r > 0 if local_row < 0 else r < lax.axis_size(axis) - 1
    return edge.astype(F32)


def masked(x, m):
    return x if m is None else x * m


def load_weights(w, k, wbuf, sems):
    copies = [pltpu.make_async_copy(w.at[k, dy], wbuf.at[dy], sems.at[dy]) for dy in range(3)]
    for c in copies:
        c.start()
    return copies


def run_conv(row_at, n_in, a3, wbuf, waits, c_ref, at, lo, strip, sums=None, squares=None):
    cols, ch = c_ref.shape[1:]
    n_out = n_in - 2
    filled = done = 0
    while done < n_out:
        rows = min(STEP, n_out - done)
        while filled < min(n_in, done + rows + 2 + AHEAD):
            put_row(a3, filled, row_at(filled))
            filled += 1
        while waits:
            waits.pop(0).wait()
        acc = conv_block(a3, wbuf, done, rows)
        c_ref[at + done : at + done + rows] = acc.reshape(rows, cols, ch)
        own_from = max(0, -(lo + done))
        own_to = min(rows, strip - (lo + done))
        if own_to > own_from:
            own = acc[own_from * cols : own_to * cols]
            s, q = fold8(own), fold8(own * own)
            sums = s if sums is None else sums + s
            squares = q if squares is None else squares + q
        done += rows
    return sums, squares


def proj_kernel(tok, w, bias, top, bot, tbuf, wbuf, sems):
    rows = tok.shape[0]
    cw = pltpu.make_async_copy(w, wbuf, sems.at[rows])
    cw.start()
    copies = [pltpu.make_async_copy(tok.at[i], tbuf.at[i], sems.at[i]) for i in range(rows)]
    for c in copies:
        c.start()
    cw.wait()
    half = rows // 2
    for i in range(0, rows, 2):
        copies[i].wait()
        copies[i + 1].wait()
        x = tbuf[i : i + 2].reshape(-1, tok.shape[2])
        y = jnp.dot(x, wbuf[...], preferred_element_type=F32) + bias[...]
        y = y.astype(BF).reshape(2, tok.shape[1], -1)
        if i < half:
            top[i : i + 2] = y
        else:
            bot[i - half : i - half + 2] = y


def relu_row(x):
    return jnp.maximum(x.astype(F32), 0.0)


def conv0_inner_kernel(top, bot, w, c_ref, wbuf, part, a3, sems, *, strip):
    waits = load_weights(w, 0, wbuf, sems)

    def row_at(i):
        return relu_row(top[i] if i < HALO else bot[i - HALO])

    sums, squares = run_conv(row_at, strip, a3, wbuf, waits, c_ref, HALO, 1, strip)
    part[0] = sums
    part[1] = squares


def conv0_outer_kernel(before, top, bot, after, wbuf, part, c_in, c_ref, st, a3, *, strip):
    sums, squares = part[0], part[1]

    def upper(i):
        return relu_row(before[i] if i < HALO else top[i - HALO])

    sums, squares = run_conv(upper, HALO + 2, a3, wbuf, [], c_ref, 0, 1 - HALO, strip, sums, squares)

    def lower(i):
        return relu_row(bot[i + HALO - 2] if i < 2 else after[i - 2])

    sums, squares = run_conv(
        lower, HALO + 2, a3, wbuf, [], c_ref, strip + HALO - 2, strip - 1, strip, sums, squares
    )
    write_stats(st, sums, squares)


def hidden_conv_kernel(c_in, stats, gain, shift, w, c_ref, st, a3, wbuf, sems, *, k, lo, n_in, strip, total, axis):
    waits = load_weights(w, k + 1, wbuf, sems)
    mean, scale, bias = norm_terms(stats, gain, shift, k, total)

    def row_at(i):
        x = jnp.maximum((c_in[i] - mean) * scale + bias, 0.0)
        return masked(x, inside(lo + i, strip, axis))

    sums, squares = run_conv(row_at, n_in, a3, wbuf, waits, c_ref, 0, lo + 1, strip)
    write_stats(st, sums, squares)


def joined_conv_kernel(
    c_in, stats, gain, shift, before, top, bot, after, w, c_ref, st, joined, a3, wbuf, sems,
    *, k, lo, n_in, strip, total, axis
):
    waits = load_weights(w, k + 1, wbuf, sems)
    mean, scale, bias = norm_terms(stats, gain, shift, k, total)
    parts = (before, top, bot, after)

    def row_at(i):
        local = lo + i
        f = parts[(local + HALO) // HALO][(local + HALO) % HALO].astype(F32)
        y = (f + ((c_in[i] - mean) * scale + bias)).astype(BF)
        if 0 <= local < strip:
            joined[local] = y
        return masked(relu_row(y), inside(local, strip, axis))

    sums, squares = run_conv(row_at, n_in, a3, wbuf, waits, c_ref, 0, lo + 1, strip)
    write_stats(st, sums, squares)


def final_kernel(joined, c_in, stats, gain, shift, out, *, k, total):
    mean, scale, bias = norm_terms(stats, gain, shift, k, total)
    for i in range(out.shape[0]):
        out[i] = (joined[i].astype(F32) + ((c_in[i] - mean) * scale + bias)).astype(BF)


def sent_to_all(value, axis):
    return lax.all_to_all(value, axis, 0, 0, tiled=True)


def reduce_all(partial):
    near = sent_to_all(partial, "row").sum(axis=0)
    far = lax.axis_size("img")
    return sent_to_all(jnp.broadcast_to(near[None], (far, *near.shape)), "img")


def on_device(tokens, proj_weight, proj_bias, conv_weight, bn_gain, bn_bias):
    imgs, strip, cols, embed = tokens.shape
    ch = proj_weight.shape[1]
    nrow = lax.axis_size("row")
    total = float(lax.axis_size("img") * nrow * imgs * strip * cols)
    weights = in_hbm(conv_weight)
    norm_args = (bn_gain, bn_bias)

    half = sds((HALO, cols, ch), BF)
    top, bot = pl.pallas_call(
        proj_kernel,
        out_shape=(half, half),
        in_specs=[HBM, HBM, VM],
        out_specs=(VM, VM),
        scratch_shapes=[
            pltpu.VMEM((strip, cols, embed), BF),
            pltpu.VMEM((embed, ch), BF),
            pltpu.SemaphoreType.DMA((strip + 1,)),
        ],
        compiler_params=PARAMS,
    )(in_hbm(tokens[0]), in_hbm(proj_weight), proj_bias[None])
    before = lax.ppermute(bot, "row", [(i, i + 1) for i in range(nrow - 1)])
    after = lax.ppermute(top, "row", [(i + 1, i) for i in range(nrow - 1)])
    top, bot, before, after = map(in_vmem, (top, bot, before, after))

    field = sds((strip + 2 * HALO - 2, cols, ch), F32)
    stat = sds((nrow, 1, 2 * ch), F32)
    wshape = (3, 3, ch, ch)

    def rows_scratch(rows):
        return pltpu.VMEM((rows, cols, 3 * ch), BF)

    wsems = pltpu.SemaphoreType.DMA((3,))
    c0, w0, part = pl.pallas_call(
        functools.partial(conv0_inner_kernel, strip=strip),
        out_shape=(field, sds(wshape, BF), sds((2, 8, ch), F32)),
        in_specs=[VM, VM, HBM],
        out_specs=(VM, VM, VM),
        scratch_shapes=[rows_scratch(strip), wsems],
        compiler_params=PARAMS,
        cost_estimate=pl.CostEstimate(
            flops=2 * 9 * ch * ch * cols * (strip - 2), transcendentals=0, bytes_accessed=9 * ch * ch * 2
        ),
    )(top, bot, weights)
    c0, st = pl.pallas_call(
        functools.partial(conv0_outer_kernel, strip=strip),
        out_shape=(field, stat),
        in_specs=[VM] * 7,
        out_specs=(VM, VM),
        input_output_aliases={6: 0},
        scratch_shapes=[rows_scratch(HALO + 2)],
        compiler_params=PARAMS,
    )(before, top, bot, after, in_vmem(w0), in_vmem(part), in_vmem(c0))

    def call(kernel, c, st, features, extra_out, n_in, **kw):
        args = (in_vmem(c), in_vmem(st), *norm_args, *features)
        return pl.pallas_call(
            functools.partial(kernel, n_in=n_in, strip=strip, total=total, axis="row", **kw),
            out_shape=(field, stat, *extra_out),
            in_specs=[VM] * len(args) + [HBM],
            out_specs=(VM,) * (2 + len(extra_out)),
            input_output_aliases={0: 0},
            scratch_shapes=[rows_scratch(n_in), pltpu.VMEM(wshape, BF), wsems],
            compiler_params=PARAMS,
        )(*args, weights)

    st = reduce_all(st)
    c1, st = call(hidden_conv_kernel, c0, st, (), (), strip + 6, k=0, lo=-3)
    st = reduce_all(st)
    c2, st, joined = call(
        joined_conv_kernel, c1, st, (before, top, bot, after), (sds((strip, cols, ch), BF),), strip + 4, k=1, lo=-2
    )
    st = reduce_all(st)
    c3, st = call(hidden_conv_kernel, c2, st, (), (), strip + 2, k=2, lo=-1)
    st = reduce_all(st)
    out = pl.pallas_call(
        functools.partial(final_kernel, k=3, total=total),
        out_shape=sds((strip, cols, ch), BF),
        in_specs=[VM] * 5,
        out_specs=VM,
        compiler_params=PARAMS,
    )(in_vmem(joined), in_vmem(c3), in_vmem(st), *norm_args)
    return out[None]


def solution(mesh):
    placed = (P("img", "row", None, None), P(), P(), P(), P(), P())
    return jax.shard_map(
        on_device, mesh=mesh, in_specs=placed, out_specs=P("img", "row", None, None), check_vma=False
    )
```

```python
import functools

import jax
import jax.numpy as jnp
from jax import lax
from jax.experimental import pallas as pl
from jax.experimental.pallas import tpu as pltpu
from jax.sharding import PartitionSpec as P

EPS = 1e-05
HALO = 4
STEP = 2
PROWS = 8
TROWS = 1
DELAY = 0
LATE = 0
AHEAD = 0
VM = pl.BlockSpec(memory_space=pltpu.VMEM)
HBM = pl.BlockSpec(memory_space=pltpu.HBM)
BF = jnp.bfloat16
F32 = jnp.float32
PARAMS = pltpu.CompilerParams(vmem_limit_bytes=24 << 20)


def sds(shape, dtype):
    return jax.ShapeDtypeStruct(shape, dtype)


def in_hbm(x):
    return pltpu.with_memory_space_constraint(x, pltpu.HBM)


def in_vmem(x):
    return pltpu.with_memory_space_constraint(x, pltpu.VMEM)


def put_row(a3, row, x):
    cols, ch = x.shape
    col = lax.broadcasted_iota(jnp.int32, x.shape, 0)
    a3[row, :, ch : 2 * ch] = x.astype(BF)
    a3[row, :, 0:ch] = jnp.where(col == 0, 0.0, pltpu.roll(x, 1, 0)).astype(BF)
    a3[row, :, 2 * ch :] = jnp.where(col == cols - 1, 0.0, pltpu.roll(x, cols - 1, 0)).astype(BF)


def fold8(x):
    return x.reshape(-1, 8, x.shape[-1]).sum(axis=0)


def norm_terms(stats_ref, gain_ref, bias_ref, k, total):
    s = jnp.sum(stats_ref[...], axis=0)
    ch = s.shape[-1] // 2
    mean = s[:, :ch] / total
    spread = jnp.maximum(s[:, ch:] / total - mean * mean, 0.0)
    return mean, lax.rsqrt(spread + EPS) * gain_ref[k : k + 1, :], bias_ref[k : k + 1, :]


def write_stats(out_ref, sums, squares):
    both = jnp.concatenate(
        [jnp.sum(sums, axis=0, keepdims=True), jnp.sum(squares, axis=0, keepdims=True)], axis=1
    )
    out_ref[...] = jnp.broadcast_to(both[None], out_ref.shape)


def inside(local_row, strip, axis):
    if 0 <= local_row < strip:
        return None
    r = lax.axis_index(axis)
    edge = r > 0 if local_row < 0 else r < lax.axis_size(axis) - 1
    return edge.astype(F32)


def masked(x, m):
    return x if m is None else x * m


def run_conv(row_at, n_in, a3, w_parts, waits, c_ref, at, lo, strip, sums=None, squares=None, starts=((), ())):
    cols, ch = c_ref.shape[1:]
    n_out = n_in - 2
    filled = 0
    for dy in range(3):
        for copy in waits[dy]:
            copy.wait()
        for copy in starts[dy - 1] if dy else ():
            copy.start()
        w = w_parts[dy][...].reshape(3 * ch, ch)
        for done in range(0, n_out, STEP):
            rows = min(STEP, n_out - done)
            while filled < min(n_in, done + rows + dy + AHEAD):
                put_row(a3, filled, row_at(filled))
                filled += 1
            lhs = a3[done + dy : done + dy + rows].reshape(rows * cols, 3 * ch)
            acc = jnp.dot(lhs, w, preferred_element_type=F32)
            into = slice(at + done, at + done + rows)
            if dy:
                acc = acc + c_ref[into].reshape(rows * cols, ch)
            c_ref[into] = acc.reshape(rows, cols, ch)
            own_from = max(0, -(lo + done))
            own_to = min(rows, strip - (lo + done))
            if dy == 2 and own_to > own_from:
                own = acc[own_from * cols : own_to * cols]
                s, q = fold8(own), fold8(own * own)
                sums = s if sums is None else sums + s
                squares = q if squares is None else squares + q
    return sums, squares


def proj_kernel(tok, w, bias, top, bot, tbuf, wbuf, bbuf, sems):
    rows = tok.shape[0]
    first = [pltpu.make_async_copy(w, wbuf, sems.at[rows]), pltpu.make_async_copy(bias, bbuf, sems.at[rows + 1])]
    copies = [
        pltpu.make_async_copy(tok.at[i : i + TROWS], tbuf.at[i : i + TROWS], sems.at[i]) for i in range(0, rows, TROWS)
    ]
    for c in first:
        c.start()
    for i, c in enumerate(copies):
        if DELAY and i * TROWS == rows // 2:
            pl.delay(DELAY)
        c.start()
    for c in first:
        c.wait()
    half = rows // 2
    for i in range(0, rows, PROWS):
        for c in copies[i // TROWS : (i + PROWS + TROWS - 1) // TROWS]:
            c.wait()
        x = tbuf[i : i + PROWS].reshape(-1, tok.shape[2])
        y = jnp.dot(x, wbuf[...], preferred_element_type=F32) + bbuf[...]
        y = y.astype(BF).reshape(PROWS, tok.shape[1], -1)
        for j in range(PROWS):
            (top if i + j < half else bot)[(i + j) % half] = y[j]


def relu_row(x):
    return jnp.maximum(x.astype(F32), 0.0)


def conv0_inner_kernel(top, bot, cw, c_ref, part, w0, a3, sems, *, strip):
    waits = [[pltpu.make_async_copy(cw.at[0, dy], w0.at[dy], sems.at[dy])] for dy in range(3)]
    for (copy,) in waits:
        copy.start()

    def row_at(i):
        return relu_row(top[i] if i < HALO else bot[i - HALO])

    w_parts = [w0.at[dy] for dy in range(3)]
    part[0], part[1] = run_conv(row_at, strip, a3, w_parts, waits, c_ref, HALO, 1, strip)


def conv0_outer_kernel(before, top, bot, after, w0, part, c_in, cw, c_ref, st, feature, w_next, a3, sem, *, strip):
    late = pltpu.make_async_copy(cw.at[1, 0], w_next, sem)
    late.start()
    w_parts = [w0.at[dy] for dy in range(3)]

    def upper(i):
        return relu_row(before[i] if i < HALO else top[i - HALO])

    sums, squares = run_conv(
        upper, HALO + 2, a3.at[: HALO + 2], w_parts, [[]] * 3, c_ref, 0, 1 - HALO, strip, part[0], part[1]
    )

    def lower(i):
        return relu_row(bot[i + HALO - 2] if i < 2 else after[i - 2])

    sums, squares = run_conv(
        lower, HALO + 2, a3.at[HALO + 2 :], w_parts, [[]] * 3, c_ref, strip + HALO - 2, strip - 1, strip, sums, squares
    )
    write_stats(st, sums, squares)
    feature[0:2] = before[HALO - 2 :]
    feature[2 : HALO + 2] = top[...]
    feature[HALO + 2 : strip + 2] = bot[...]
    feature[strip + 2 :] = after[0:2]
    late.wait()


def weight_copies(cw, k, wbuf, w_next, sems):
    waits = [[]] + [[pltpu.make_async_copy(cw.at[k, dy], wbuf.at[dy - 1], sems.at[dy - 1])] for dy in (1, 2)]
    late = []
    if w_next is not None:
        late.append(pltpu.make_async_copy(cw.at[k + 1, 0], w_next, sems.at[2]))
    for c in waits[1]:
        c.start()
    after = [waits[2], [], []]
    after[LATE] = after[LATE] + late
    for c in after[0]:
        c.start()
    return waits, late, after[1:]


def hidden_conv_kernel(
    c_in, stats, gain, shift, w_first, cw, c_ref, st, *rest, k, lo, n_in, strip, total, axis
):
    *w_next, a3, wbuf, sems = rest
    waits, late, starts = weight_copies(cw, k + 1, wbuf, w_next[0] if w_next else None, sems)
    mean, scale, bias = norm_terms(stats, gain, shift, k, total)

    def row_at(i):
        x = jnp.maximum((c_in[i] - mean) * scale + bias, 0.0)
        return masked(x, inside(lo + i, strip, axis))

    w_parts = [w_first, wbuf.at[0], wbuf.at[1]]
    write_stats(st, *run_conv(row_at, n_in, a3, w_parts, waits, c_ref, 0, lo + 1, strip, starts=starts))
    for c in late:
        c.wait()


def joined_conv_kernel(
    c_in, stats, gain, shift, w_first, feature, cw, c_ref, st, w_next, joined, a3, wbuf, sems,
    *, k, lo, n_in, strip, total, axis
):
    waits, late, starts = weight_copies(cw, k + 1, wbuf, w_next, sems)
    mean, scale, bias = norm_terms(stats, gain, shift, k, total)

    def row_at(i):
        y = (feature[i].astype(F32) + ((c_in[i] - mean) * scale + bias)).astype(BF)
        joined[i] = y
        return masked(relu_row(y), inside(lo + i, strip, axis))

    w_parts = [w_first, wbuf.at[0], wbuf.at[1]]
    write_stats(st, *run_conv(row_at, n_in, a3, w_parts, waits, c_ref, 0, lo + 1, strip, starts=starts))
    for c in late:
        c.wait()


def final_kernel(joined, c_in, stats, gain, shift, out, *, k, total):
    mean, scale, bias = norm_terms(stats, gain, shift, k, total)
    for i in range(out.shape[0]):
        out[i] = (joined[i + 2].astype(F32) + ((c_in[i] - mean) * scale + bias)).astype(BF)


def sent_to_all(value, axis):
    return lax.all_to_all(value, axis, 0, 0, tiled=True)


def reduce_all(partial):
    near = sent_to_all(partial, "row").sum(axis=0)
    far = lax.axis_size("img")
    return sent_to_all(jnp.broadcast_to(near[None], (far, *near.shape)), "img")


def on_device(tokens, proj_weight, proj_bias, conv_weight, bn_gain, bn_bias):
    imgs, strip, cols, embed = tokens.shape
    ch = proj_weight.shape[1]
    nrow = lax.axis_size("row")
    total = float(lax.axis_size("img") * nrow * imgs * strip * cols)
    weights = in_hbm(conv_weight)
    norm_args = (bn_gain, bn_bias)

    half = sds((HALO, cols, ch), BF)
    w_third = sds((3, ch, ch), BF)
    top, bot = pl.pallas_call(
        proj_kernel,
        out_shape=(half, half),
        in_specs=[HBM] * 3,
        out_specs=(VM, VM),
        scratch_shapes=[
            pltpu.VMEM((strip, cols, embed), BF),
            pltpu.VMEM((embed, ch), BF),
            pltpu.VMEM((1, ch), F32),
            pltpu.SemaphoreType.DMA((strip + 2,)),
        ],
        compiler_params=PARAMS,
    )(in_hbm(tokens[0]), in_hbm(proj_weight), in_hbm(proj_bias[None]))
    before = lax.ppermute(bot, "row", [(i, i + 1) for i in range(nrow - 1)])
    after = lax.ppermute(top, "row", [(i + 1, i) for i in range(nrow - 1)])
    top, bot, before, after = map(in_vmem, (top, bot, before, after))

    field = sds((strip + 2 * HALO - 2, cols, ch), F32)
    stat = sds((nrow, 1, 2 * ch), F32)
    context = sds((strip + 4, cols, ch), BF)

    def rows_scratch(rows):
        return pltpu.VMEM((rows, cols, 3 * ch), BF)

    c0, part, w0 = pl.pallas_call(
        functools.partial(conv0_inner_kernel, strip=strip),
        out_shape=(field, sds((2, 8, ch), F32), sds((3, 3, ch, ch), BF)),
        in_specs=[VM, VM, HBM],
        out_specs=(VM,) * 3,
        scratch_shapes=[rows_scratch(strip), pltpu.SemaphoreType.DMA((3,))],
        compiler_params=PARAMS,
        cost_estimate=pl.CostEstimate(
            flops=2 * 9 * ch * ch * cols * (strip - 2), transcendentals=0, bytes_accessed=9 * ch * ch * 2
        ),
    )(top, bot, weights)
    c, st, feature, w_next = pl.pallas_call(
        functools.partial(conv0_outer_kernel, strip=strip),
        out_shape=(field, stat, context, w_third),
        in_specs=[VM] * 7 + [HBM],
        out_specs=(VM,) * 4,
        input_output_aliases={6: 0},
        scratch_shapes=[rows_scratch(2 * HALO + 4), pltpu.SemaphoreType.DMA(())],
        compiler_params=PARAMS,
    )(before, top, bot, after, in_vmem(w0), in_vmem(part), in_vmem(c0), weights)

    def call(kernel, extra_in, extra_out, n_in, aliases, **kw):
        args = (in_vmem(c), in_vmem(st), *norm_args, *map(in_vmem, extra_in))
        return pl.pallas_call(
            functools.partial(kernel, n_in=n_in, strip=strip, total=total, axis="row", **kw),
            out_shape=(field, stat, *extra_out),
            in_specs=[VM] * len(args) + [HBM],
            out_specs=(VM,) * (2 + len(extra_out)),
            input_output_aliases={0: 0, **aliases},
            scratch_shapes=[
                rows_scratch(n_in),
                pltpu.VMEM((2, 3, ch, ch), BF),
                pltpu.SemaphoreType.DMA((3,)),
            ],
            compiler_params=PARAMS,
        )(*args, weights)

    st = reduce_all(st)
    c, st, w_next = call(hidden_conv_kernel, (w_next,), (w_third,), strip + 6, {}, k=0, lo=-3)
    st = reduce_all(st)
    c, st, w_next, joined = call(
        joined_conv_kernel, (w_next, feature), (w_third, context), strip + 4, {5: 3}, k=1, lo=-2
    )
    st = reduce_all(st)
    c, st = call(hidden_conv_kernel, (w_next,), (), strip + 2, {}, k=2, lo=-1)
    st = reduce_all(st)
    out = pl.pallas_call(
        functools.partial(final_kernel, k=3, total=total),
        out_shape=sds((strip, cols, ch), BF),
        in_specs=[VM] * 5,
        out_specs=VM,
        compiler_params=PARAMS,
    )(in_vmem(joined), in_vmem(c), in_vmem(st), *norm_args)
    return out[None]


def solution(mesh):
    placed = (P("img", "row", None, None), P(), P(), P(), P(), P())
    return jax.shard_map(
        on_device, mesh=mesh, in_specs=placed, out_specs=P("img", "row", None, None), check_vma=False
    )
```

```python
import functools

import jax
import jax.numpy as jnp
from jax import lax
from jax.experimental import pallas as pl
from jax.experimental.pallas import tpu as pltpu
from jax.sharding import PartitionSpec as P

EPS = 1e-05
HALO = 4
STEP = 2
LATE = 0
AHEAD = 0
VM = pl.BlockSpec(memory_space=pltpu.VMEM)
HBM = pl.BlockSpec(memory_space=pltpu.HBM)
BF = jnp.bfloat16
F32 = jnp.float32
PARAMS = pltpu.CompilerParams(vmem_limit_bytes=24 << 20)


def sds(shape, dtype):
    return jax.ShapeDtypeStruct(shape, dtype)


def in_hbm(x):
    return pltpu.with_memory_space_constraint(x, pltpu.HBM)


def in_vmem(x):
    return pltpu.with_memory_space_constraint(x, pltpu.VMEM)


def put_row(a3, row, x):
    cols, ch = x.shape
    col = lax.broadcasted_iota(jnp.int32, x.shape, 0)
    a3[row, :, ch : 2 * ch] = x.astype(BF)
    a3[row, :, 0:ch] = jnp.where(col == 0, 0.0, pltpu.roll(x, 1, 0)).astype(BF)
    a3[row, :, 2 * ch :] = jnp.where(col == cols - 1, 0.0, pltpu.roll(x, cols - 1, 0)).astype(BF)


def fold8(x):
    return x.reshape(-1, 8, x.shape[-1]).sum(axis=0)


def norm_terms(stats_ref, gain_ref, bias_ref, k, total):
    s = jnp.sum(stats_ref[...], axis=0)
    ch = s.shape[-1] // 2
    mean = s[:, :ch] / total
    spread = jnp.maximum(s[:, ch:] / total - mean * mean, 0.0)
    return mean, lax.rsqrt(spread + EPS) * gain_ref[k : k + 1, :], bias_ref[k : k + 1, :]


def write_stats(out_ref, sums, squares):
    both = jnp.concatenate(
        [jnp.sum(sums, axis=0, keepdims=True), jnp.sum(squares, axis=0, keepdims=True)], axis=1
    )
    out_ref[...] = jnp.broadcast_to(both[None], out_ref.shape)


def inside(local_row, strip, axis):
    if 0 <= local_row < strip:
        return None
    r = lax.axis_index(axis)
    edge = r > 0 if local_row < 0 else r < lax.axis_size(axis) - 1
    return edge.astype(F32)


def masked(x, m):
    return x if m is None else x * m


def run_conv(row_at, n_in, a3, w_parts, waits, c_ref, at, lo, strip, sums=None, squares=None, starts=((), ())):
    cols, ch = c_ref.shape[1:]
    n_out = n_in - 2
    filled = 0
    for dy in range(3):
        for copy in waits[dy]:
            copy.wait()
        for copy in starts[dy - 1] if dy else ():
            copy.start()
        w = w_parts[dy][...].reshape(3 * ch, ch)
        for done in range(0, n_out, STEP):
            rows = min(STEP, n_out - done)
            while filled < min(n_in, done + rows + dy + AHEAD):
                put_row(a3, filled, row_at(filled))
                filled += 1
            lhs = a3[done + dy : done + dy + rows].reshape(rows * cols, 3 * ch)
            acc = jnp.dot(lhs, w, preferred_element_type=F32)
            into = slice(at + done, at + done + rows)
            if dy:
                acc = acc + c_ref[into].reshape(rows * cols, ch)
            c_ref[into] = acc.reshape(rows, cols, ch)
            own_from = max(0, -(lo + done))
            own_to = min(rows, strip - (lo + done))
            if dy == 2 and own_to > own_from:
                own = acc[own_from * cols : own_to * cols]
                s, q = fold8(own), fold8(own * own)
                sums = s if sums is None else sums + s
                squares = q if squares is None else squares + q
    return sums, squares


def near_is_top(axis):
    return lax.axis_index(axis) % 2 == 1


def proj_kernel(tok, w, bias, far, near, tbuf, wbuf, bbuf, sems, *, axis):
    rows = tok.shape[0]
    near_at = jnp.where(near_is_top(axis), 0, HALO)
    copies = [
        pltpu.make_async_copy(w, wbuf, sems.at[0]),
        pltpu.make_async_copy(bias, bbuf, sems.at[1]),
        pltpu.make_async_copy(tok.at[pl.ds(HALO - near_at, HALO)], tbuf.at[0:HALO], sems.at[2]),
        pltpu.make_async_copy(tok.at[pl.ds(near_at, HALO)], tbuf.at[HALO:], sems.at[3]),
    ]
    for c in copies:
        c.start()
    for c in copies:
        c.wait()
    y = jnp.dot(tbuf[...].reshape(-1, tok.shape[2]), wbuf[...], preferred_element_type=F32) + bbuf[...]
    y = y.astype(BF).reshape(rows, tok.shape[1], -1)
    far[...] = y[:HALO]
    near[...] = y[HALO:]


def relu_row(x):
    return jnp.maximum(x.astype(F32), 0.0)


def pick(cond, a, b):
    return jnp.where(cond, a.astype(F32), b.astype(F32))


def conv0_inner_kernel(far, near, cw, c_ref, part, w0, a3, sems, *, strip, axis):
    waits = [[pltpu.make_async_copy(cw.at[0, dy], w0.at[dy], sems.at[dy])] for dy in range(3)]
    for (copy,) in waits:
        copy.start()
    flip = near_is_top(axis)

    def row_at(i):
        j = i % HALO
        return relu_row(pick(flip, near[j], far[j]) if i < HALO else pick(flip, far[j], near[j]))

    w_parts = [w0.at[dy] for dy in range(3)]
    part[0], part[1] = run_conv(row_at, strip, a3, w_parts, waits, c_ref, HALO, 1, strip)


def conv0_outer_kernel(
    got_far, far, near, got_near, w0, part, c_in, cw, c_ref, st, feature, w_next, a3, sem, *, strip, axis
):
    late = pltpu.make_async_copy(cw.at[1, 0], w_next, sem)
    late.start()
    w_parts = [w0.at[dy] for dy in range(3)]
    flip = near_is_top(axis)

    def strip_row(i):
        j = i % HALO
        if i < 0:
            return pick(flip, got_near[j], got_far[j])
        if i < HALO:
            return pick(flip, near[j], far[j])
        if i < strip:
            return pick(flip, far[j], near[j])
        return pick(flip, got_far[j], got_near[j])

    def upper(i):
        return relu_row(strip_row(i - HALO))

    def lower(i):
        return relu_row(strip_row(strip - 2 + i))

    sums, squares = run_conv(
        upper, HALO + 2, a3.at[: HALO + 2], w_parts, [[]] * 3, c_ref, 0, 1 - HALO, strip, part[0], part[1]
    )
    sums, squares = run_conv(
        lower, HALO + 2, a3.at[HALO + 2 :], w_parts, [[]] * 3, c_ref, strip + HALO - 2, strip - 1, strip, sums, squares
    )
    write_stats(st, sums, squares)
    for i in range(feature.shape[0]):
        feature[i] = strip_row(i - 2).astype(BF)
    late.wait()


def weight_copies(cw, k, wbuf, w_next, sems):
    waits = [[]] + [[pltpu.make_async_copy(cw.at[k, dy], wbuf.at[dy - 1], sems.at[dy - 1])] for dy in (1, 2)]
    late = []
    if w_next is not None:
        late.append(pltpu.make_async_copy(cw.at[k + 1, 0], w_next, sems.at[2]))
    for c in waits[1]:
        c.start()
    after = [waits[2], [], []]
    after[LATE] = after[LATE] + late
    for c in after[0]:
        c.start()
    return waits, late, after[1:]


def hidden_conv_kernel(
    c_in, stats, gain, shift, w_first, cw, c_ref, st, *rest, k, lo, n_in, strip, total, axis
):
    *w_next, a3, wbuf, sems = rest
    waits, late, starts = weight_copies(cw, k + 1, wbuf, w_next[0] if w_next else None, sems)
    mean, scale, bias = norm_terms(stats, gain, shift, k, total)

    def row_at(i):
        x = jnp.maximum((c_in[i] - mean) * scale + bias, 0.0)
        return masked(x, inside(lo + i, strip, axis))

    w_parts = [w_first, wbuf.at[0], wbuf.at[1]]
    write_stats(st, *run_conv(row_at, n_in, a3, w_parts, waits, c_ref, 0, lo + 1, strip, starts=starts))
    for c in late:
        c.wait()


def joined_conv_kernel(
    c_in, stats, gain, shift, w_first, feature, cw, c_ref, st, w_next, joined, a3, wbuf, sems,
    *, k, lo, n_in, strip, total, axis
):
    waits, late, starts = weight_copies(cw, k + 1, wbuf, w_next, sems)
    mean, scale, bias = norm_terms(stats, gain, shift, k, total)

    def row_at(i):
        y = (feature[i].astype(F32) + ((c_in[i] - mean) * scale + bias)).astype(BF)
        joined[i] = y
        return masked(relu_row(y), inside(lo + i, strip, axis))

    w_parts = [w_first, wbuf.at[0], wbuf.at[1]]
    write_stats(st, *run_conv(row_at, n_in, a3, w_parts, waits, c_ref, 0, lo + 1, strip, starts=starts))
    for c in late:
        c.wait()


def final_kernel(joined, c_in, stats, gain, shift, out, *, k, total):
    mean, scale, bias = norm_terms(stats, gain, shift, k, total)
    for i in range(out.shape[0]):
        out[i] = (joined[i + 2].astype(F32) + ((c_in[i] - mean) * scale + bias)).astype(BF)


def sent_to_all(value, axis):
    return lax.all_to_all(value, axis, 0, 0, tiled=True)


def reduce_all(partial):
    near = sent_to_all(partial, "row").sum(axis=0)
    far = lax.axis_size("img")
    return sent_to_all(jnp.broadcast_to(near[None], (far, *near.shape)), "img")


def swapped(value, firsts):
    pairs = [(i, i + 1) for i in firsts]
    return lax.ppermute(value, "row", pairs + [(j, i) for i, j in pairs])


def on_device(tokens, proj_weight, proj_bias, conv_weight, bn_gain, bn_bias):
    imgs, strip, cols, embed = tokens.shape
    ch = proj_weight.shape[1]
    nrow = lax.axis_size("row")
    total = float(lax.axis_size("img") * nrow * imgs * strip * cols)
    weights = in_hbm(conv_weight)
    norm_args = (bn_gain, bn_bias)

    half = sds((HALO, cols, ch), BF)
    w_third = sds((3, ch, ch), BF)
    far, near = pl.pallas_call(
        functools.partial(proj_kernel, axis="row"),
        out_shape=(half, half),
        in_specs=[HBM] * 3,
        out_specs=(VM, VM),
        scratch_shapes=[
            pltpu.VMEM((strip, cols, embed), BF),
            pltpu.VMEM((embed, ch), BF),
            pltpu.VMEM((1, ch), F32),
            pltpu.SemaphoreType.DMA((4,)),
        ],
        compiler_params=PARAMS,
    )(in_hbm(tokens[0]), in_hbm(proj_weight), in_hbm(proj_bias[None]))
    got_far = swapped(far, range(1, nrow - 1, 2))
    got_near = swapped(near, range(0, nrow - 1, 2))
    far, near, got_far, got_near = map(in_vmem, (far, near, got_far, got_near))

    field = sds((strip + 2 * HALO - 2, cols, ch), F32)
    stat = sds((nrow, 1, 2 * ch), F32)
    context = sds((strip + 4, cols, ch), BF)

    def rows_scratch(rows):
        return pltpu.VMEM((rows, cols, 3 * ch), BF)

    c0, part, w0 = pl.pallas_call(
        functools.partial(conv0_inner_kernel, strip=strip, axis="row"),
        out_shape=(field, sds((2, 8, ch), F32), sds((3, 3, ch, ch), BF)),
        in_specs=[VM, VM, HBM],
        out_specs=(VM,) * 3,
        scratch_shapes=[rows_scratch(strip), pltpu.SemaphoreType.DMA((3,))],
        compiler_params=PARAMS,
        cost_estimate=pl.CostEstimate(
            flops=2 * 9 * ch * ch * cols * (strip - 2), transcendentals=0, bytes_accessed=9 * ch * ch * 2
        ),
    )(far, near, weights)
    c, st, feature, w_next = pl.pallas_call(
        functools.partial(conv0_outer_kernel, strip=strip, axis="row"),
        out_shape=(field, stat, context, w_third),
        in_specs=[VM] * 7 + [HBM],
        out_specs=(VM,) * 4,
        input_output_aliases={6: 0},
        scratch_shapes=[rows_scratch(2 * HALO + 4), pltpu.SemaphoreType.DMA(())],
        compiler_params=PARAMS,
    )(got_far, far, near, got_near, in_vmem(w0), in_vmem(part), in_vmem(c0), weights)

    def call(kernel, extra_in, extra_out, n_in, aliases, **kw):
        args = (in_vmem(c), in_vmem(st), *norm_args, *map(in_vmem, extra_in))
        return pl.pallas_call(
            functools.partial(kernel, n_in=n_in, strip=strip, total=total, axis="row", **kw),
            out_shape=(field, stat, *extra_out),
            in_specs=[VM] * len(args) + [HBM],
            out_specs=(VM,) * (2 + len(extra_out)),
            input_output_aliases={0: 0, **aliases},
            scratch_shapes=[
                rows_scratch(n_in),
                pltpu.VMEM((2, 3, ch, ch), BF),
                pltpu.SemaphoreType.DMA((3,)),
            ],
            compiler_params=PARAMS,
        )(*args, weights)

    st = reduce_all(st)
    c, st, w_next = call(hidden_conv_kernel, (w_next,), (w_third,), strip + 6, {}, k=0, lo=-3)
    st = reduce_all(st)
    c, st, w_next, joined = call(
        joined_conv_kernel, (w_next, feature), (w_third, context), strip + 4, {5: 3}, k=1, lo=-2
    )
    st = reduce_all(st)
    c, st = call(hidden_conv_kernel, (w_next,), (), strip + 2, {}, k=2, lo=-1)
    st = reduce_all(st)
    out = pl.pallas_call(
        functools.partial(final_kernel, k=3, total=total),
        out_shape=sds((strip, cols, ch), BF),
        in_specs=[VM] * 5,
        out_specs=VM,
        compiler_params=PARAMS,
    )(in_vmem(joined), in_vmem(c), in_vmem(st), *norm_args)
    return out[None]


def solution(mesh):
    placed = (P("img", "row", None, None), P(), P(), P(), P(), P())
    return jax.shard_map(
        on_device, mesh=mesh, in_specs=placed, out_specs=P("img", "row", None, None), check_vma=False
    )
```

```python
import functools

import jax
import jax.numpy as jnp
from jax import lax
from jax.experimental import pallas as pl
from jax.experimental.pallas import tpu as pltpu
from jax.sharding import PartitionSpec as P

EPS = 1e-05
HALO = 4
SHAPES = {'inner': (3, 0), 'outer': (2, 0), 0: (2, 0), 1: (5, 0), 2: (2, 0)}
VM = pl.BlockSpec(memory_space=pltpu.VMEM)
HBM = pl.BlockSpec(memory_space=pltpu.HBM)
BF = jnp.bfloat16
F32 = jnp.float32
PARAMS = pltpu.CompilerParams(vmem_limit_bytes=24 << 20)


def sds(shape, dtype):
    return jax.ShapeDtypeStruct(shape, dtype)


def in_hbm(x):
    return pltpu.with_memory_space_constraint(x, pltpu.HBM)


def in_vmem(x):
    return pltpu.with_memory_space_constraint(x, pltpu.VMEM)


def put_row(a3, row, x):
    cols, ch = x.shape
    col = lax.broadcasted_iota(jnp.int32, x.shape, 0)
    a3[row, :, ch : 2 * ch] = x.astype(BF)
    a3[row, :, 0:ch] = jnp.where(col == 0, 0.0, pltpu.roll(x, 1, 0)).astype(BF)
    a3[row, :, 2 * ch :] = jnp.where(col == cols - 1, 0.0, pltpu.roll(x, cols - 1, 0)).astype(BF)


def fold8(x):
    return x.reshape(-1, 8, x.shape[-1]).sum(axis=0)


def norm_terms(stats_ref, gain_ref, bias_ref, k, total):
    s = jnp.sum(stats_ref[...], axis=0)
    ch = s.shape[-1] // 2
    mean = s[:, :ch] / total
    spread = jnp.maximum(s[:, ch:] / total - mean * mean, 0.0)
    return mean, lax.rsqrt(spread + EPS) * gain_ref[k : k + 1, :], bias_ref[k : k + 1, :]


def write_stats(out_ref, sums, squares):
    both = jnp.concatenate(
        [jnp.sum(sums, axis=0, keepdims=True), jnp.sum(squares, axis=0, keepdims=True)], axis=1
    )
    out_ref[...] = jnp.broadcast_to(both[None], out_ref.shape)


def inside(local_row, strip, axis):
    if 0 <= local_row < strip:
        return None
    r = lax.axis_index(axis)
    edge = r > 0 if local_row < 0 else r < lax.axis_size(axis) - 1
    return edge.astype(F32)


def masked(x, m):
    return x if m is None else x * m


def run_conv(row_at, n_in, a3, w_parts, waits, c_ref, at, lo, strip, sums=None, squares=None, tile=(2, 0)):
    cols, ch = c_ref.shape[1:]
    n_out = n_in - 2
    step, ahead = tile
    filled = 0
    for dy in range(3):
        for copy in waits[dy]:
            copy.wait()
        w = w_parts[dy][...].reshape(3 * ch, ch)
        for done in range(0, n_out, step):
            rows = min(step, n_out - done)
            while filled < min(n_in, done + rows + dy + ahead):
                put_row(a3, filled, row_at(filled))
                filled += 1
            lhs = a3[done + dy : done + dy + rows].reshape(rows * cols, 3 * ch)
            acc = jnp.dot(lhs, w, preferred_element_type=F32)
            into = slice(at + done, at + done + rows)
            if dy:
                acc = acc + c_ref[into].reshape(rows * cols, ch)
            c_ref[into] = acc.reshape(rows, cols, ch)
            own_from = max(0, -(lo + done))
            own_to = min(rows, strip - (lo + done))
            if dy == 2 and own_to > own_from:
                own = acc[own_from * cols : own_to * cols]
                s, q = fold8(own), fold8(own * own)
                sums = s if sums is None else sums + s
                squares = q if squares is None else squares + q
    return sums, squares


def near_is_top(axis):
    return lax.axis_index(axis) % 2 == 1


def proj_kernel(tok, w, bias, far, near, tbuf, wbuf, bbuf, sems, *, axis):
    rows = tok.shape[0]
    near_at = jnp.where(near_is_top(axis), 0, HALO)
    copies = [
        pltpu.make_async_copy(w, wbuf, sems.at[0]),
        pltpu.make_async_copy(bias, bbuf, sems.at[1]),
        pltpu.make_async_copy(tok.at[pl.ds(HALO - near_at, HALO)], tbuf.at[0:HALO], sems.at[2]),
        pltpu.make_async_copy(tok.at[pl.ds(near_at, HALO)], tbuf.at[HALO:], sems.at[3]),
    ]
    for c in copies:
        c.start()
    for c in copies:
        c.wait()
    y = jnp.dot(tbuf[...].reshape(-1, tok.shape[2]), wbuf[...], preferred_element_type=F32) + bbuf[...]
    y = y.astype(BF).reshape(rows, tok.shape[1], -1)
    far[...] = y[:HALO]
    near[...] = y[HALO:]


def relu_row(x):
    return jnp.maximum(x.astype(F32), 0.0)


def pick(cond, a, b):
    return jnp.where(cond, a.astype(F32), b.astype(F32))


def conv0_inner_kernel(far, near, cw, c_ref, part, w0, a3, sems, *, strip, axis):
    waits = [[pltpu.make_async_copy(cw.at[0, dy], w0.at[dy], sems.at[dy])] for dy in range(3)]
    for (copy,) in waits:
        copy.start()
    flip = near_is_top(axis)

    def row_at(i):
        j = i % HALO
        return relu_row(pick(flip, near[j], far[j]) if i < HALO else pick(flip, far[j], near[j]))

    w_parts = [w0.at[dy] for dy in range(3)]
    part[0], part[1] = run_conv(row_at, strip, a3, w_parts, waits, c_ref, HALO, 1, strip, tile=SHAPES['inner'])


def conv0_outer_kernel(
    got_far, far, near, got_near, w0, part, c_in, cw, c_ref, st, feature, w_next, a3, sem, *, strip, axis
):
    late = pltpu.make_async_copy(cw.at[1, 0], w_next, sem)
    late.start()
    w_parts = [w0.at[dy] for dy in range(3)]
    flip = near_is_top(axis)

    def strip_row(i):
        j = i % HALO
        if i < 0:
            return pick(flip, got_near[j], got_far[j])
        if i < HALO:
            return pick(flip, near[j], far[j])
        if i < strip:
            return pick(flip, far[j], near[j])
        return pick(flip, got_far[j], got_near[j])

    def upper(i):
        return relu_row(strip_row(i - HALO))

    def lower(i):
        return relu_row(strip_row(strip - 2 + i))

    sums, squares = run_conv(
        upper, HALO + 2, a3.at[: HALO + 2], w_parts, [[]] * 3, c_ref, 0, 1 - HALO, strip, part[0], part[1],
        tile=SHAPES['outer'],
    )
    sums, squares = run_conv(
        lower, HALO + 2, a3.at[HALO + 2 :], w_parts, [[]] * 3, c_ref, strip + HALO - 2, strip - 1, strip, sums, squares,
        tile=SHAPES['outer'],
    )
    write_stats(st, sums, squares)
    for i in range(feature.shape[0]):
        feature[i] = strip_row(i - 2).astype(BF)
    late.wait()


def weight_copies(cw, k, wbuf, w_next, sems):
    waits = [[]] + [[pltpu.make_async_copy(cw.at[k, dy], wbuf.at[dy - 1], sems.at[dy - 1])] for dy in (1, 2)]
    late = []
    if w_next is not None:
        late.append(pltpu.make_async_copy(cw.at[k + 1, 0], w_next, sems.at[2]))
    for c in waits[1]:
        c.start()
    for c in waits[2] + late:
        c.start()
    return waits, late


def hidden_conv_kernel(
    c_in, stats, gain, shift, w_first, cw, c_ref, st, *rest, k, lo, n_in, strip, total, axis
):
    *w_next, a3, wbuf, sems = rest
    waits, late = weight_copies(cw, k + 1, wbuf, w_next[0] if w_next else None, sems)
    mean, scale, bias = norm_terms(stats, gain, shift, k, total)

    def row_at(i):
        x = jnp.maximum((c_in[i] - mean) * scale + bias, 0.0)
        return masked(x, inside(lo + i, strip, axis))

    w_parts = [w_first, wbuf.at[0], wbuf.at[1]]
    write_stats(st, *run_conv(row_at, n_in, a3, w_parts, waits, c_ref, 0, lo + 1, strip, tile=SHAPES[k]))
    for c in late:
        c.wait()


def joined_conv_kernel(
    c_in, stats, gain, shift, w_first, feature, cw, c_ref, st, w_next, joined, a3, wbuf, sems,
    *, k, lo, n_in, strip, total, axis
):
    waits, late = weight_copies(cw, k + 1, wbuf, w_next, sems)
    mean, scale, bias = norm_terms(stats, gain, shift, k, total)

    def row_at(i):
        y = (feature[i].astype(F32) + ((c_in[i] - mean) * scale + bias)).astype(BF)
        joined[i] = y
        return masked(relu_row(y), inside(lo + i, strip, axis))

    w_parts = [w_first, wbuf.at[0], wbuf.at[1]]
    write_stats(st, *run_conv(row_at, n_in, a3, w_parts, waits, c_ref, 0, lo + 1, strip, tile=SHAPES[k]))
    for c in late:
        c.wait()


def final_kernel(joined, c_in, stats, gain, shift, out, rows, sems, *, k, total):
    mean, scale, bias = norm_terms(stats, gain, shift, k, total)
    copies = []
    for i in range(0, rows.shape[0], 2):
        for j in (i, i + 1):
            rows[j] = (joined[j + 2].astype(F32) + ((c_in[j] - mean) * scale + bias)).astype(BF)
        copies.append(pltpu.make_async_copy(rows.at[i : i + 2], out.at[i : i + 2], sems.at[i // 2]))
        copies[-1].start()
    for c in copies:
        c.wait()


def sent_to_all(value, axis):
    return lax.all_to_all(value, axis, 0, 0, tiled=True)


def reduce_all(partial):
    near = sent_to_all(partial, "row").sum(axis=0)
    far = lax.axis_size("img")
    return sent_to_all(jnp.broadcast_to(near[None], (far, *near.shape)), "img")


def swapped(value, firsts):
    pairs = [(i, i + 1) for i in firsts]
    return lax.ppermute(value, "row", pairs + [(j, i) for i, j in pairs])


def on_device(tokens, proj_weight, proj_bias, conv_weight, bn_gain, bn_bias):
    imgs, strip, cols, embed = tokens.shape
    ch = proj_weight.shape[1]
    nrow = lax.axis_size("row")
    total = float(lax.axis_size("img") * nrow * imgs * strip * cols)
    weights = in_hbm(conv_weight)
    norm_args = (bn_gain, bn_bias)

    half = sds((HALO, cols, ch), BF)
    w_third = sds((3, ch, ch), BF)
    far, near = pl.pallas_call(
        functools.partial(proj_kernel, axis="row"),
        out_shape=(half, half),
        in_specs=[HBM] * 3,
        out_specs=(VM, VM),
        scratch_shapes=[
            pltpu.VMEM((strip, cols, embed), BF),
            pltpu.VMEM((embed, ch), BF),
            pltpu.VMEM((1, ch), F32),
            pltpu.SemaphoreType.DMA((4,)),
        ],
        compiler_params=PARAMS,
    )(in_hbm(tokens[0]), in_hbm(proj_weight), in_hbm(proj_bias[None]))
    got_far = swapped(far, range(1, nrow - 1, 2))
    got_near = swapped(near, range(0, nrow - 1, 2))
    far, near, got_far, got_near = map(in_vmem, (far, near, got_far, got_near))

    field = sds((strip + 2 * HALO - 2, cols, ch), F32)
    stat = sds((nrow, 1, 2 * ch), F32)
    context = sds((strip + 4, cols, ch), BF)

    def rows_scratch(rows):
        return pltpu.VMEM((rows, cols, 3 * ch), BF)

    c0, part, w0 = pl.pallas_call(
        functools.partial(conv0_inner_kernel, strip=strip, axis="row"),
        out_shape=(field, sds((2, 8, ch), F32), sds((3, 3, ch, ch), BF)),
        in_specs=[VM, VM, HBM],
        out_specs=(VM,) * 3,
        scratch_shapes=[rows_scratch(strip), pltpu.SemaphoreType.DMA((3,))],
        compiler_params=PARAMS,
        cost_estimate=pl.CostEstimate(
            flops=2 * 9 * ch * ch * cols * (strip - 2), transcendentals=0, bytes_accessed=9 * ch * ch * 2
        ),
    )(far, near, weights)
    c, st, feature, w_next = pl.pallas_call(
        functools.partial(conv0_outer_kernel, strip=strip, axis="row"),
        out_shape=(field, stat, context, w_third),
        in_specs=[VM] * 7 + [HBM],
        out_specs=(VM,) * 4,
        input_output_aliases={6: 0},
        scratch_shapes=[rows_scratch(2 * HALO + 4), pltpu.SemaphoreType.DMA(())],
        compiler_params=PARAMS,
    )(got_far, far, near, got_near, in_vmem(w0), in_vmem(part), in_vmem(c0), weights)

    def call(kernel, extra_in, extra_out, n_in, aliases, **kw):
        args = (in_vmem(c), in_vmem(st), *norm_args, *map(in_vmem, extra_in))
        return pl.pallas_call(
            functools.partial(kernel, n_in=n_in, strip=strip, total=total, axis="row", **kw),
            out_shape=(field, stat, *extra_out),
            in_specs=[VM] * len(args) + [HBM],
            out_specs=(VM,) * (2 + len(extra_out)),
            input_output_aliases={0: 0, **aliases},
            scratch_shapes=[
                rows_scratch(n_in),
                pltpu.VMEM((2, 3, ch, ch), BF),
                pltpu.SemaphoreType.DMA((3,)),
            ],
            compiler_params=PARAMS,
        )(*args, weights)

    st = reduce_all(st)
    c, st, w_next = call(hidden_conv_kernel, (w_next,), (w_third,), strip + 6, {}, k=0, lo=-3)
    st = reduce_all(st)
    c, st, w_next, joined = call(
        joined_conv_kernel, (w_next, feature), (w_third, context), strip + 4, {5: 3}, k=1, lo=-2
    )
    st = reduce_all(st)
    c, st = call(hidden_conv_kernel, (w_next,), (), strip + 2, {}, k=2, lo=-1)
    st = reduce_all(st)
    out = pl.pallas_call(
        functools.partial(final_kernel, k=3, total=total),
        out_shape=sds((strip, cols, ch), BF),
        in_specs=[VM] * 5,
        out_specs=HBM,
        scratch_shapes=[pltpu.VMEM((strip, cols, ch), BF), pltpu.SemaphoreType.DMA((strip // 2,))],
        compiler_params=PARAMS,
    )(in_vmem(joined), in_vmem(c), in_vmem(st), *norm_args)
    return out[None]


def solution(mesh):
    placed = (P("img", "row", None, None), P(), P(), P(), P(), P())
    return jax.shard_map(
        on_device, mesh=mesh, in_specs=placed, out_specs=P("img", "row", None, None), check_vma=False
    )
```

```python
import functools

import jax
import jax.numpy as jnp
from jax import lax
from jax.experimental import pallas as pl
from jax.experimental.pallas import tpu as pltpu
from jax.sharding import PartitionSpec as P


EPS = 1e-05
HALO = 4
SHAPES = {'inner': (3, 0), 'outer': (2, 0), 0: (2, 0), 1: (5, 0), 2: (2, 0)}
VM = pl.BlockSpec(memory_space=pltpu.VMEM)
HBM = pl.BlockSpec(memory_space=pltpu.HBM)
BF = jnp.bfloat16
F32 = jnp.float32
PARAMS = pltpu.CompilerParams(vmem_limit_bytes=24 << 20)


def sds(shape, dtype):
    return jax.ShapeDtypeStruct(shape, dtype)


def in_hbm(x):
    return pltpu.with_memory_space_constraint(x, pltpu.HBM)


def in_vmem(x):
    return pltpu.with_memory_space_constraint(x, pltpu.VMEM)


def put_row(a3, row, x):
    cols, ch = x.shape
    col = lax.broadcasted_iota(jnp.int32, x.shape, 0)
    a3[row, :, ch : 2 * ch] = x.astype(BF)
    a3[row, :, 0:ch] = jnp.where(col == 0, 0.0, pltpu.roll(x, 1, 0)).astype(BF)
    a3[row, :, 2 * ch :] = jnp.where(col == cols - 1, 0.0, pltpu.roll(x, cols - 1, 0)).astype(BF)


def fold8(x):
    return x.reshape(-1, 8, x.shape[-1]).sum(axis=0)


def norm_terms(stats_ref, gain_ref, bias_ref, k, total):
    s = jnp.sum(stats_ref[...], axis=0)
    ch = s.shape[-1] // 2
    mean = s[:, :ch] / total
    spread = jnp.maximum(s[:, ch:] / total - mean * mean, 0.0)
    return mean, lax.rsqrt(spread + EPS) * gain_ref[k : k + 1, :], bias_ref[k : k + 1, :]


def write_stats(out_ref, sums, squares):
    both = jnp.concatenate(
        [jnp.sum(sums, axis=0, keepdims=True), jnp.sum(squares, axis=0, keepdims=True)], axis=1
    )
    out_ref[...] = jnp.broadcast_to(both[None], out_ref.shape)


def inside(local_row, strip, axis):
    if 0 <= local_row < strip:
        return None
    r = lax.axis_index(axis)
    edge = r > 0 if local_row < 0 else r < lax.axis_size(axis) - 1
    return edge.astype(F32)


def masked(x, m):
    return x if m is None else x * m


def run_conv(row_at, n_in, a3, w_parts, waits, c_ref, at, lo, strip, sums=None, squares=None, tile=(2, 0)):
    cols, ch = c_ref.shape[1:]
    n_out = n_in - 2
    step, ahead = tile
    filled = 0
    for dy in range(3):
        for copy in waits[dy]:
            copy.wait()
        w = w_parts[dy][...].reshape(3 * ch, ch)
        for done in range(0, n_out, step):
            rows = min(step, n_out - done)
            while filled < min(n_in, done + rows + dy + ahead):
                put_row(a3, filled, row_at(filled))
                filled += 1
            lhs = a3[done + dy : done + dy + rows].reshape(rows * cols, 3 * ch)
            acc = jnp.dot(lhs, w, preferred_element_type=F32)
            into = pl.ds(at + done, rows)
            if dy:
                acc = acc + c_ref[into].reshape(rows * cols, ch)
            c_ref[into] = acc.reshape(rows, cols, ch)
            own_from = max(0, -(lo + done))
            own_to = min(rows, strip - (lo + done))
            if dy == 2 and own_to > own_from:
                own = acc[own_from * cols : own_to * cols]
                s, q = fold8(own), fold8(own * own)
                sums = s if sums is None else sums + s
                squares = q if squares is None else squares + q
    return sums, squares


def near_is_top(axis):
    return lax.axis_index(axis) % 2 == 1


def project(tbuf, wbuf, bbuf, out):
    y = jnp.dot(tbuf[...].reshape(-1, tbuf.shape[2]), wbuf[...], preferred_element_type=F32) + bbuf[...]
    out[...] = y.astype(BF).reshape(out.shape)


def far_proj_kernel(tok, w, bias, far, wbuf, bbuf, tbuf, sems, *, axis):
    far_at = jnp.where(near_is_top(axis), HALO, 0)
    copies = [
        pltpu.make_async_copy(w, wbuf, sems.at[0]),
        pltpu.make_async_copy(bias, bbuf, sems.at[1]),
        pltpu.make_async_copy(tok.at[pl.ds(far_at, HALO)], tbuf, sems.at[2]),
    ]
    for c in copies:
        c.start()
    for c in copies:
        c.wait()
    project(tbuf, wbuf, bbuf, far)


def near_proj_kernel(wbuf, bbuf, tok, near, tbuf, sem, *, axis):
    copy = pltpu.make_async_copy(tok.at[pl.ds(jnp.where(near_is_top(axis), 0, HALO), HALO)], tbuf, sem)
    copy.start()
    copy.wait()
    project(tbuf, wbuf, bbuf, near)


def relu_row(x):
    return jnp.maximum(x.astype(F32), 0.0)


def pick(cond, a, b):
    return jnp.where(cond, a.astype(F32), b.astype(F32))


def conv0_inner_kernel(far, near, cw, c_ref, part, w0, w_next, a3, sems, *, strip, axis):
    waits = [[pltpu.make_async_copy(cw.at[0, dy], w0.at[dy], sems.at[dy])] for dy in range(3)]
    late = pltpu.make_async_copy(cw.at[1, 0], w_next, sems.at[3])
    for copy in (*waits[0], *waits[1], *waits[2], late):
        copy.start()
    flip = near_is_top(axis)

    def row_at(i):
        j = i % HALO
        return relu_row(pick(flip, near[j], far[j]) if i < HALO else pick(flip, far[j], near[j]))

    w_parts = [w0.at[dy] for dy in range(3)]
    part[0], part[1] = run_conv(row_at, strip, a3, w_parts, waits, c_ref, HALO, 1, strip, tile=SHAPES["inner"])
    late.wait()


def conv0_edge(got, own, w0, part, c_ref, a3, upper, strip):
    def row_at(i):
        above = got[i] if i < HALO else own[i - HALO]
        below = own[i + HALO - 2] if i < 2 else got[i - 2]
        return relu_row(pick(upper, above, below))

    w_parts = [w0.at[dy] for dy in range(3)]
    at = jnp.where(upper, 0, strip + HALO - 2)
    run_conv(row_at, HALO + 2, a3, w_parts, [[]] * 3, c_ref, at, strip, strip, tile=SHAPES["outer"])
    row = c_ref[jnp.where(upper, HALO - 1, strip + HALO - 2)]
    return part[0] + fold8(row), part[1] + fold8(row * row)


def conv0_near_kernel(got, far, near, w0, part_in, c_in, c_ref, part, feature, a3, *, strip, axis):
    flip = near_is_top(axis)
    part[0], part[1] = conv0_edge(got, near, w0, part_in, c_ref, a3, flip, strip)
    near_at = jnp.where(flip, 0, HALO)
    feature[pl.ds(2 + near_at, HALO)] = near[...]
    feature[pl.ds(2 + HALO - near_at, HALO)] = far[...]
    feature[pl.ds(jnp.where(flip, 0, strip + 2), 2)] = got[pl.ds(jnp.where(flip, HALO - 2, 0), 2)]


def conv0_far_kernel(got, far, w0, part, c_in, feature_in, c_ref, st, feature, a3, *, strip, axis):
    flip = near_is_top(axis)
    upper = jnp.logical_not(flip)
    sums, squares = conv0_edge(got, far, w0, part, c_ref, a3, upper, strip)
    write_stats(st, sums, squares)
    feature[pl.ds(jnp.where(flip, strip + 2, 0), 2)] = got[pl.ds(jnp.where(flip, 0, HALO - 2), 2)]


def weight_copies(cw, k, wbuf, w_next, sems):
    waits = [[]] + [[pltpu.make_async_copy(cw.at[k, dy], wbuf.at[dy - 1], sems.at[dy - 1])] for dy in (1, 2)]
    late = []
    if w_next is not None:
        late.append(pltpu.make_async_copy(cw.at[k + 1, 0], w_next, sems.at[2]))
    for c in waits[1]:
        c.start()
    for c in waits[2] + late:
        c.start()
    return waits, late


def hidden_conv_kernel(
    c_in, stats, gain, shift, w_first, cw, c_ref, st, *rest, k, lo, n_in, strip, total, axis
):
    *w_next, a3, wbuf, sems = rest
    waits, late = weight_copies(cw, k + 1, wbuf, w_next[0] if w_next else None, sems)
    mean, scale, bias = norm_terms(stats, gain, shift, k, total)

    def row_at(i):
        x = jnp.maximum((c_in[i] - mean) * scale + bias, 0.0)
        return masked(x, inside(lo + i, strip, axis))

    w_parts = [w_first, wbuf.at[0], wbuf.at[1]]
    write_stats(st, *run_conv(row_at, n_in, a3, w_parts, waits, c_ref, 0, lo + 1, strip, tile=SHAPES[k]))
    for c in late:
        c.wait()


def joined_conv_kernel(
    c_in, stats, gain, shift, w_first, feature, cw, c_ref, st, w_next, joined, a3, wbuf, sems,
    *, k, lo, n_in, strip, total, axis
):
    waits, late = weight_copies(cw, k + 1, wbuf, w_next, sems)
    mean, scale, bias = norm_terms(stats, gain, shift, k, total)

    def row_at(i):
        y = (feature[i].astype(F32) + ((c_in[i] - mean) * scale + bias)).astype(BF)
        joined[i] = y
        return masked(relu_row(y), inside(lo + i, strip, axis))

    w_parts = [w_first, wbuf.at[0], wbuf.at[1]]
    write_stats(st, *run_conv(row_at, n_in, a3, w_parts, waits, c_ref, 0, lo + 1, strip, tile=SHAPES[k]))
    for c in late:
        c.wait()


def final_kernel(joined, c_in, stats, gain, shift, out, rows, sems, *, k, total):
    mean, scale, bias = norm_terms(stats, gain, shift, k, total)
    copies = []
    for i in range(0, rows.shape[0], 2):
        for j in (i, i + 1):
            rows[j] = (joined[j + 2].astype(F32) + ((c_in[j] - mean) * scale + bias)).astype(BF)
        copies.append(pltpu.make_async_copy(rows.at[i : i + 2], out.at[i : i + 2], sems.at[i // 2]))
        copies[-1].start()
    for c in copies:
        c.wait()


def sent_to_all(value, axis):
    return lax.all_to_all(value, axis, 0, 0, tiled=True)


def reduce_all(partial):
    near = sent_to_all(partial, "row").sum(axis=0)
    far = lax.axis_size("img")
    return sent_to_all(jnp.broadcast_to(near[None], (far, *near.shape)), "img")


def swapped(value, firsts):
    pairs = [(i, i + 1) for i in firsts]
    return lax.ppermute(value, "row", pairs + [(j, i) for i, j in pairs])


def on_device(tokens, proj_weight, proj_bias, conv_weight, bn_gain, bn_bias):
    imgs, strip, cols, embed = tokens.shape
    ch = proj_weight.shape[1]
    nrow = lax.axis_size("row")
    total = float(lax.axis_size("img") * nrow * imgs * strip * cols)
    weights = in_hbm(conv_weight)
    norm_args = (bn_gain, bn_bias)

    half = sds((HALO, cols, ch), BF)
    w_third = sds((3, ch, ch), BF)
    token_rows = in_hbm(tokens[0])
    far, pw, pb = pl.pallas_call(
        functools.partial(far_proj_kernel, axis="row"),
        out_shape=(half, sds((embed, ch), BF), sds((1, ch), F32)),
        in_specs=[HBM] * 3,
        out_specs=(VM,) * 3,
        scratch_shapes=[pltpu.VMEM((HALO, cols, embed), BF), pltpu.SemaphoreType.DMA((3,))],
        compiler_params=PARAMS,
    )(token_rows, in_hbm(proj_weight), in_hbm(proj_bias[None]))
    got_far = swapped(far, range(1, nrow - 1, 2))
    near_call = pl.pallas_call(
        functools.partial(near_proj_kernel, axis="row"),
        out_shape=half,
        in_specs=[VM, VM, HBM],
        out_specs=VM,
        scratch_shapes=[pltpu.VMEM((HALO, cols, embed), BF), pltpu.SemaphoreType.DMA(())],
        compiler_params=PARAMS,
        cost_estimate=pl.CostEstimate(
            flops=2 * embed * ch * cols * HALO, transcendentals=0, bytes_accessed=2 * HALO * cols * embed
        ),
    )
    near = near_call(in_vmem(pw), in_vmem(pb), token_rows)
    got_near = swapped(near, range(0, nrow - 1, 2))
    far, near, got_far, got_near = map(in_vmem, (far, near, got_far, got_near))

    field = sds((strip + 2 * HALO - 2, cols, ch), F32)
    stat = sds((nrow, 1, 2 * ch), F32)
    context = sds((strip + 4, cols, ch), BF)

    def rows_scratch(rows):
        return pltpu.VMEM((rows, cols, 3 * ch), BF)

    sums = sds((2, 8, ch), F32)

    def conv_flops(rows):
        return pl.CostEstimate(
            flops=2 * 9 * ch * ch * cols * rows, transcendentals=0, bytes_accessed=9 * ch * ch * 2
        )

    c, part, w0, w_next = pl.pallas_call(
        functools.partial(conv0_inner_kernel, strip=strip, axis="row"),
        out_shape=(field, sums, sds((3, 3, ch, ch), BF), w_third),
        in_specs=[VM, VM, HBM],
        out_specs=(VM,) * 4,
        scratch_shapes=[rows_scratch(strip), pltpu.SemaphoreType.DMA((4,))],
        compiler_params=PARAMS,
        cost_estimate=conv_flops(strip - 2),
    )(far, near, weights)
    w0 = in_vmem(w0)
    c, part, feature = pl.pallas_call(
        functools.partial(conv0_near_kernel, strip=strip, axis="row"),
        out_shape=(field, sums, context),
        in_specs=[VM] * 6,
        out_specs=(VM,) * 3,
        input_output_aliases={5: 0},
        scratch_shapes=[rows_scratch(HALO + 2)],
        compiler_params=PARAMS,
        cost_estimate=conv_flops(HALO),
    )(got_near, far, near, w0, in_vmem(part), in_vmem(c))
    c, st, feature = pl.pallas_call(
        functools.partial(conv0_far_kernel, strip=strip, axis="row"),
        out_shape=(field, stat, context),
        in_specs=[VM] * 6,
        out_specs=(VM,) * 3,
        input_output_aliases={4: 0, 5: 2},
        scratch_shapes=[rows_scratch(HALO + 2)],
        compiler_params=PARAMS,
        cost_estimate=conv_flops(HALO),
    )(got_far, far, w0, in_vmem(part), in_vmem(c), in_vmem(feature))

    def call(kernel, extra_in, extra_out, n_in, aliases, **kw):
        args = (in_vmem(c), in_vmem(st), *norm_args, *map(in_vmem, extra_in))
        return pl.pallas_call(
            functools.partial(kernel, n_in=n_in, strip=strip, total=total, axis="row", **kw),
            out_shape=(field, stat, *extra_out),
            in_specs=[VM] * len(args) + [HBM],
            out_specs=(VM,) * (2 + len(extra_out)),
            input_output_aliases={0: 0, **aliases},
            scratch_shapes=[
                rows_scratch(n_in),
                pltpu.VMEM((2, 3, ch, ch), BF),
                pltpu.SemaphoreType.DMA((3,)),
            ],
            compiler_params=PARAMS,
        )(*args, weights)

    st = reduce_all(st)
    c, st, w_next = call(hidden_conv_kernel, (w_next,), (w_third,), strip + 6, {}, k=0, lo=-3)
    st = reduce_all(st)
    c, st, w_next, joined = call(
        joined_conv_kernel, (w_next, feature), (w_third, context), strip + 4, {5: 3}, k=1, lo=-2
    )
    st = reduce_all(st)
    c, st = call(hidden_conv_kernel, (w_next,), (), strip + 2, {}, k=2, lo=-1)
    st = reduce_all(st)
    out = pl.pallas_call(
        functools.partial(final_kernel, k=3, total=total),
        out_shape=sds((strip, cols, ch), BF),
        in_specs=[VM] * 5,
        out_specs=HBM,
        scratch_shapes=[pltpu.VMEM((strip, cols, ch), BF), pltpu.SemaphoreType.DMA((strip // 2,))],
        compiler_params=PARAMS,
    )(in_vmem(joined), in_vmem(c), in_vmem(st), *norm_args)
    return out[None]


def solution(mesh):
    placed = (P("img", "row", None, None), P(), P(), P(), P(), P())
    return jax.shard_map(
        on_device, mesh=mesh, in_specs=placed, out_specs=P("img", "row", None, None), check_vma=False
    )
```

```python
import functools

import jax
import jax.numpy as jnp
from jax import lax
from jax.experimental import pallas as pl
from jax.experimental.pallas import tpu as pltpu
from jax.sharding import PartitionSpec as P


EPS = 1e-05
HALO = 4
SHAPES = {'inner': (3, 0), 'outer': (2, 0), 0: (2, 0), 1: (5, 0), 2: (2, 0)}
VM = pl.BlockSpec(memory_space=pltpu.VMEM)
HBM = pl.BlockSpec(memory_space=pltpu.HBM)
BF = jnp.bfloat16
F32 = jnp.float32
PARAMS = pltpu.CompilerParams(vmem_limit_bytes=24 << 20)


def sds(shape, dtype):
    return jax.ShapeDtypeStruct(shape, dtype)


def in_hbm(x):
    return pltpu.with_memory_space_constraint(x, pltpu.HBM)


def in_vmem(x):
    return pltpu.with_memory_space_constraint(x, pltpu.VMEM)


def put_row(a3, row, x):
    cols, ch = x.shape
    col = lax.broadcasted_iota(jnp.int32, x.shape, 0)
    a3[row, :, ch : 2 * ch] = x.astype(BF)
    a3[row, :, 0:ch] = jnp.where(col == 0, 0.0, pltpu.roll(x, 1, 0)).astype(BF)
    a3[row, :, 2 * ch :] = jnp.where(col == cols - 1, 0.0, pltpu.roll(x, cols - 1, 0)).astype(BF)


def fold8(x):
    return x.reshape(-1, 8, x.shape[-1]).sum(axis=0)


def norm_terms(stats_ref, gain_ref, bias_ref, k, total):
    s = jnp.sum(stats_ref[...], axis=0)
    ch = s.shape[-1] // 2
    mean = s[:, :ch] / total
    spread = jnp.maximum(s[:, ch:] / total - mean * mean, 0.0)
    return mean, lax.rsqrt(spread + EPS) * gain_ref[k : k + 1, :], bias_ref[k : k + 1, :]


def write_stats(out_ref, sums, squares):
    both = jnp.concatenate(
        [jnp.sum(sums, axis=0, keepdims=True), jnp.sum(squares, axis=0, keepdims=True)], axis=1
    )
    out_ref[...] = jnp.broadcast_to(both[None], out_ref.shape)


def inside(local_row, strip, axis):
    if 0 <= local_row < strip:
        return None
    r = lax.axis_index(axis)
    edge = r > 0 if local_row < 0 else r < lax.axis_size(axis) - 1
    return edge.astype(F32)


def masked(x, m):
    return x if m is None else x * m


def run_conv(row_at, n_in, a3, w_parts, waits, c_ref, at, lo, strip, sums=None, squares=None, tile=(2, 0)):
    cols, ch = c_ref.shape[1:]
    n_out = n_in - 2
    step, ahead = tile
    filled = 0
    for dy in range(3):
        for copy in waits[dy]:
            copy.wait()
        w = w_parts[dy][...].reshape(3 * ch, ch)
        for done in range(0, n_out, step):
            rows = min(step, n_out - done)
            while filled < min(n_in, done + rows + dy + ahead):
                put_row(a3, filled, row_at(filled))
                filled += 1
            lhs = a3[done + dy : done + dy + rows].reshape(rows * cols, 3 * ch)
            acc = jnp.dot(lhs, w, preferred_element_type=F32)
            into = pl.ds(at + done, rows)
            if dy:
                acc = acc + c_ref[into].reshape(rows * cols, ch)
            c_ref[into] = acc.reshape(rows, cols, ch)
            own_from = max(0, -(lo + done))
            own_to = min(rows, strip - (lo + done))
            if dy == 2 and own_to > own_from:
                own = acc[own_from * cols : own_to * cols]
                s, q = fold8(own), fold8(own * own)
                sums = s if sums is None else sums + s
                squares = q if squares is None else squares + q
    return sums, squares


def near_is_top(axis):
    return lax.axis_index(axis) % 2 == 1


def project(tbuf, wbuf, bbuf, out):
    y = jnp.dot(tbuf[...].reshape(-1, tbuf.shape[2]), wbuf[...], preferred_element_type=F32) + bbuf[...]
    out[...] = y.astype(BF).reshape(out.shape)


def far_proj_kernel(tok, w, bias, far, wbuf, bbuf, tbuf, sems, *, axis):
    far_at = jnp.where(near_is_top(axis), HALO, 0)
    copies = [
        pltpu.make_async_copy(w, wbuf, sems.at[0]),
        pltpu.make_async_copy(bias, bbuf, sems.at[1]),
        pltpu.make_async_copy(tok.at[pl.ds(far_at, HALO)], tbuf, sems.at[2]),
    ]
    for c in copies:
        c.start()
    for c in copies:
        c.wait()
    project(tbuf, wbuf, bbuf, far)


def near_proj_kernel(wbuf, bbuf, tok, near, tbuf, sem, *, axis):
    copy = pltpu.make_async_copy(tok.at[pl.ds(jnp.where(near_is_top(axis), 0, HALO), HALO)], tbuf, sem)
    copy.start()
    copy.wait()
    project(tbuf, wbuf, bbuf, near)


def relu_row(x):
    return jnp.maximum(x.astype(F32), 0.0)


def pick(cond, a, b):
    return jnp.where(cond, a.astype(F32), b.astype(F32))


def conv0_inner_kernel(far, near, cw, c_ref, part, w0, w_next, a3, sems, *, strip, axis):
    waits = [[pltpu.make_async_copy(cw.at[0, dy], w0.at[dy], sems.at[dy])] for dy in range(3)]
    late = pltpu.make_async_copy(cw.at[1, 0], w_next, sems.at[3])
    for copy in (*waits[0], *waits[1], *waits[2], late):
        copy.start()
    flip = near_is_top(axis)

    def row_at(i):
        j = i % HALO
        return relu_row(pick(flip, near[j], far[j]) if i < HALO else pick(flip, far[j], near[j]))

    w_parts = [w0.at[dy] for dy in range(3)]
    part[0], part[1] = run_conv(row_at, strip, a3, w_parts, waits, c_ref, HALO, 1, strip, tile=SHAPES["inner"])
    late.wait()


def conv0_edge(got, own, w0, part, c_ref, a3, upper, strip, exists=None):
    def theirs(i):
        return got[i] if exists is None else got[i].astype(F32) * exists

    def row_at(i):
        above = theirs(i) if i < HALO else own[i - HALO]
        below = own[i + HALO - 2] if i < 2 else theirs(i - 2)
        return relu_row(pick(upper, above, below))

    w_parts = [w0.at[dy] for dy in range(3)]
    at = jnp.where(upper, 0, strip + HALO - 2)
    run_conv(row_at, HALO + 2, a3, w_parts, [[]] * 3, c_ref, at, strip, strip, tile=SHAPES["outer"])
    row = c_ref[jnp.where(upper, HALO - 1, strip + HALO - 2)]
    return part[0] + fold8(row), part[1] + fold8(row * row)


def conv0_near_kernel(got, far, near, w0, part_in, c_in, c_ref, part, feature, a3, *, strip, axis):
    flip = near_is_top(axis)
    part[0], part[1] = conv0_edge(got, near, w0, part_in, c_ref, a3, flip, strip)
    near_at = jnp.where(flip, 0, HALO)
    feature[pl.ds(2 + near_at, HALO)] = near[...]
    feature[pl.ds(2 + HALO - near_at, HALO)] = far[...]
    feature[pl.ds(jnp.where(flip, 0, strip + 2), 2)] = got[pl.ds(jnp.where(flip, HALO - 2, 0), 2)]


def conv0_far_kernel(got, far, w0, part, c_in, feature_in, c_ref, st, feature, a3, *, strip, axis):
    flip = near_is_top(axis)
    upper = jnp.logical_not(flip)
    r = lax.axis_index(axis)
    exists = jnp.logical_and(r > 0, r < lax.axis_size(axis) - 1).astype(F32)
    sums, squares = conv0_edge(got, far, w0, part, c_ref, a3, upper, strip, exists)
    write_stats(st, sums, squares)
    feature[pl.ds(jnp.where(flip, strip + 2, 0), 2)] = got[pl.ds(jnp.where(flip, 0, HALO - 2), 2)]


def weight_copies(cw, k, wbuf, w_next, sems):
    waits = [[]] + [[pltpu.make_async_copy(cw.at[k, dy], wbuf.at[dy - 1], sems.at[dy - 1])] for dy in (1, 2)]
    late = []
    if w_next is not None:
        late.append(pltpu.make_async_copy(cw.at[k + 1, 0], w_next, sems.at[2]))
    for c in waits[1]:
        c.start()
    for c in waits[2] + late:
        c.start()
    return waits, late


def hidden_conv_kernel(
    c_in, stats, gain, shift, w_first, cw, c_ref, st, *rest, k, lo, n_in, strip, total, axis
):
    *w_next, a3, wbuf, sems = rest
    waits, late = weight_copies(cw, k + 1, wbuf, w_next[0] if w_next else None, sems)
    mean, scale, bias = norm_terms(stats, gain, shift, k, total)

    def row_at(i):
        x = jnp.maximum((c_in[i] - mean) * scale + bias, 0.0)
        return masked(x, inside(lo + i, strip, axis))

    w_parts = [w_first, wbuf.at[0], wbuf.at[1]]
    write_stats(st, *run_conv(row_at, n_in, a3, w_parts, waits, c_ref, 0, lo + 1, strip, tile=SHAPES[k]))
    for c in late:
        c.wait()


def joined_conv_kernel(
    c_in, stats, gain, shift, w_first, feature, cw, c_ref, st, w_next, joined, a3, wbuf, sems,
    *, k, lo, n_in, strip, total, axis
):
    waits, late = weight_copies(cw, k + 1, wbuf, w_next, sems)
    mean, scale, bias = norm_terms(stats, gain, shift, k, total)

    def row_at(i):
        y = (feature[i].astype(F32) + ((c_in[i] - mean) * scale + bias)).astype(BF)
        joined[i] = y
        return masked(relu_row(y), inside(lo + i, strip, axis))

    w_parts = [w_first, wbuf.at[0], wbuf.at[1]]
    write_stats(st, *run_conv(row_at, n_in, a3, w_parts, waits, c_ref, 0, lo + 1, strip, tile=SHAPES[k]))
    for c in late:
        c.wait()


def final_kernel(joined, c_in, stats, gain, shift, out, rows, sems, *, k, total):
    mean, scale, bias = norm_terms(stats, gain, shift, k, total)
    copies = []
    for i in range(0, rows.shape[0], 2):
        for j in (i, i + 1):
            rows[j] = (joined[j + 2].astype(F32) + ((c_in[j] - mean) * scale + bias)).astype(BF)
        copies.append(pltpu.make_async_copy(rows.at[i : i + 2], out.at[i : i + 2], sems.at[i // 2]))
        copies[-1].start()
    for c in copies:
        c.wait()


def sent_to_all(value, axis):
    return lax.all_to_all(value, axis, 0, 0, tiled=True)


def reduce_all(partial):
    near = sent_to_all(partial, "row").sum(axis=0)
    far = lax.axis_size("img")
    return sent_to_all(jnp.broadcast_to(near[None], (far, *near.shape)), "img")


def swapped(value, firsts):
    pairs = [(i, (i + 1) % lax.axis_size("row")) for i in firsts]
    return lax.ppermute(value, "row", pairs + [(j, i) for i, j in pairs])


def on_device(tokens, proj_weight, proj_bias, conv_weight, bn_gain, bn_bias):
    imgs, strip, cols, embed = tokens.shape
    ch = proj_weight.shape[1]
    nrow = lax.axis_size("row")
    total = float(lax.axis_size("img") * nrow * imgs * strip * cols)
    weights = in_hbm(conv_weight)
    norm_args = (bn_gain, bn_bias)

    half = sds((HALO, cols, ch), BF)
    w_third = sds((3, ch, ch), BF)
    token_rows = in_hbm(tokens[0])
    far, pw, pb = pl.pallas_call(
        functools.partial(far_proj_kernel, axis="row"),
        out_shape=(half, sds((embed, ch), BF), sds((1, ch), F32)),
        in_specs=[HBM] * 3,
        out_specs=(VM,) * 3,
        scratch_shapes=[pltpu.VMEM((HALO, cols, embed), BF), pltpu.SemaphoreType.DMA((3,))],
        compiler_params=PARAMS,
    )(token_rows, in_hbm(proj_weight), in_hbm(proj_bias[None]))
    got_far = swapped(far, range(1, nrow, 2))
    near_call = pl.pallas_call(
        functools.partial(near_proj_kernel, axis="row"),
        out_shape=half,
        in_specs=[VM, VM, HBM],
        out_specs=VM,
        scratch_shapes=[pltpu.VMEM((HALO, cols, embed), BF), pltpu.SemaphoreType.DMA(())],
        compiler_params=PARAMS,
        cost_estimate=pl.CostEstimate(
            flops=2 * embed * ch * cols * HALO, transcendentals=0, bytes_accessed=2 * HALO * cols * embed
        ),
    )
    near = near_call(in_vmem(pw), in_vmem(pb), token_rows)
    got_near = swapped(near, range(0, nrow - 1, 2))
    far, near, got_far, got_near = map(in_vmem, (far, near, got_far, got_near))

    field = sds((strip + 2 * HALO - 2, cols, ch), F32)
    stat = sds((nrow, 1, 2 * ch), F32)
    context = sds((strip + 4, cols, ch), BF)

    def rows_scratch(rows):
        return pltpu.VMEM((rows, cols, 3 * ch), BF)

    sums = sds((2, 8, ch), F32)

    def conv_flops(rows):
        return pl.CostEstimate(
            flops=2 * 9 * ch * ch * cols * rows, transcendentals=0, bytes_accessed=9 * ch * ch * 2
        )

    c, part, w0, w_next = pl.pallas_call(
        functools.partial(conv0_inner_kernel, strip=strip, axis="row"),
        out_shape=(field, sums, sds((3, 3, ch, ch), BF), w_third),
        in_specs=[VM, VM, HBM],
        out_specs=(VM,) * 4,
        scratch_shapes=[rows_scratch(strip), pltpu.SemaphoreType.DMA((4,))],
        compiler_params=PARAMS,
        cost_estimate=conv_flops(strip - 2),
    )(far, near, weights)
    w0 = in_vmem(w0)
    c, part, feature = pl.pallas_call(
        functools.partial(conv0_near_kernel, strip=strip, axis="row"),
        out_shape=(field, sums, context),
        in_specs=[VM] * 6,
        out_specs=(VM,) * 3,
        input_output_aliases={5: 0},
        scratch_shapes=[rows_scratch(HALO + 2)],
        compiler_params=PARAMS,
        cost_estimate=conv_flops(HALO),
    )(got_near, far, near, w0, in_vmem(part), in_vmem(c))
    c, st, feature = pl.pallas_call(
        functools.partial(conv0_far_kernel, strip=strip, axis="row"),
        out_shape=(field, stat, context),
        in_specs=[VM] * 6,
        out_specs=(VM,) * 3,
        input_output_aliases={4: 0, 5: 2},
        scratch_shapes=[rows_scratch(HALO + 2)],
        compiler_params=PARAMS,
        cost_estimate=conv_flops(HALO),
    )(got_far, far, w0, in_vmem(part), in_vmem(c), in_vmem(feature))

    def call(kernel, extra_in, extra_out, n_in, aliases, **kw):
        args = (in_vmem(c), in_vmem(st), *norm_args, *map(in_vmem, extra_in))
        return pl.pallas_call(
            functools.partial(kernel, n_in=n_in, strip=strip, total=total, axis="row", **kw),
            out_shape=(field, stat, *extra_out),
            in_specs=[VM] * len(args) + [HBM],
            out_specs=(VM,) * (2 + len(extra_out)),
            input_output_aliases={0: 0, **aliases},
            scratch_shapes=[
                rows_scratch(n_in),
                pltpu.VMEM((2, 3, ch, ch), BF),
                pltpu.SemaphoreType.DMA((3,)),
            ],
            compiler_params=PARAMS,
        )(*args, weights)

    st = reduce_all(st)
    c, st, w_next = call(hidden_conv_kernel, (w_next,), (w_third,), strip + 6, {}, k=0, lo=-3)
    st = reduce_all(st)
    c, st, w_next, joined = call(
        joined_conv_kernel, (w_next, feature), (w_third, context), strip + 4, {5: 3}, k=1, lo=-2
    )
    st = reduce_all(st)
    c, st = call(hidden_conv_kernel, (w_next,), (), strip + 2, {}, k=2, lo=-1)
    st = reduce_all(st)
    out = pl.pallas_call(
        functools.partial(final_kernel, k=3, total=total),
        out_shape=sds((strip, cols, ch), BF),
        in_specs=[VM] * 5,
        out_specs=HBM,
        scratch_shapes=[pltpu.VMEM((strip, cols, ch), BF), pltpu.SemaphoreType.DMA((strip // 2,))],
        compiler_params=PARAMS,
    )(in_vmem(joined), in_vmem(c), in_vmem(st), *norm_args)
    return out[None]


def solution(mesh):
    placed = (P("img", "row", None, None), P(), P(), P(), P(), P())
    return jax.shard_map(
        on_device, mesh=mesh, in_specs=placed, out_specs=P("img", "row", None, None), check_vma=False
    )
```

```python
import functools

import jax
import jax.numpy as jnp
from jax import lax
from jax.experimental import pallas as pl
from jax.experimental.pallas import tpu as pltpu
from jax.sharding import PartitionSpec as P


EPS = 1e-05
HALO = 2
SHAPES = {'inner': (3, 0), 'outer': (2, 0), 0: (2, 0), 1: (5, 0), 2: (2, 0)}
VM = pl.BlockSpec(memory_space=pltpu.VMEM)
HBM = pl.BlockSpec(memory_space=pltpu.HBM)
BF = jnp.bfloat16
F32 = jnp.float32
PARAMS = pltpu.CompilerParams(vmem_limit_bytes=24 << 20)


def sds(shape, dtype):
    return jax.ShapeDtypeStruct(shape, dtype)


def in_hbm(x):
    return pltpu.with_memory_space_constraint(x, pltpu.HBM)


def in_vmem(x):
    return pltpu.with_memory_space_constraint(x, pltpu.VMEM)


def put_row(a3, row, x):
    cols, ch = x.shape
    col = lax.broadcasted_iota(jnp.int32, x.shape, 0)
    a3[row, :, ch : 2 * ch] = x.astype(BF)
    a3[row, :, 0:ch] = jnp.where(col == 0, 0.0, pltpu.roll(x, 1, 0)).astype(BF)
    a3[row, :, 2 * ch :] = jnp.where(col == cols - 1, 0.0, pltpu.roll(x, cols - 1, 0)).astype(BF)


def fold8(x):
    return x.reshape(-1, 8, x.shape[-1]).sum(axis=0)


def norm_terms(stats_ref, gain_ref, bias_ref, k, total):
    s = jnp.sum(stats_ref[...], axis=0)
    ch = s.shape[-1] // 2
    mean = s[:, :ch] / total
    spread = jnp.maximum(s[:, ch:] / total - mean * mean, 0.0)
    return mean, lax.rsqrt(spread + EPS) * gain_ref[k : k + 1, :], bias_ref[k : k + 1, :]


def write_stats(out_ref, sums, squares):
    both = jnp.concatenate(
        [jnp.sum(sums, axis=0, keepdims=True), jnp.sum(squares, axis=0, keepdims=True)], axis=1
    )
    out_ref[...] = jnp.broadcast_to(both[None], out_ref.shape)


def inside(local_row, strip, axis):
    if 0 <= local_row < strip:
        return None
    r = lax.axis_index(axis)
    edge = r > 0 if local_row < 0 else r < lax.axis_size(axis) - 1
    return edge.astype(F32)


def masked(x, m):
    return x if m is None else x * m


def run_conv(row_at, n_in, a3, w_parts, waits, c_ref, at, lo, strip, sums=None, squares=None, tile=(2, 0)):
    cols, ch = c_ref.shape[1:]
    n_out = n_in - 2
    step, ahead = tile
    filled = 0
    for dy in range(3):
        for copy in waits[dy]:
            copy.wait()
        w = w_parts[dy][...].reshape(3 * ch, ch)
        for done in range(0, n_out, step):
            rows = min(step, n_out - done)
            while filled < min(n_in, done + rows + dy + ahead):
                put_row(a3, filled, row_at(filled))
                filled += 1
            lhs = a3[done + dy : done + dy + rows].reshape(rows * cols, 3 * ch)
            acc = jnp.dot(lhs, w, preferred_element_type=F32)
            into = pl.ds(at + done, rows)
            if dy:
                acc = acc + c_ref[into].reshape(rows * cols, ch)
            c_ref[into] = acc.reshape(rows, cols, ch)
            own_from = max(0, -(lo + done))
            own_to = min(rows, strip - (lo + done))
            if dy == 2 and own_to > own_from:
                own = acc[own_from * cols : own_to * cols]
                s, q = fold8(own), fold8(own * own)
                sums = s if sums is None else sums + s
                squares = q if squares is None else squares + q
    return sums, squares


def near_is_top(axis):
    return lax.axis_index(axis) % 2 == 1


def project(tbuf, wbuf, bbuf, out):
    y = jnp.dot(tbuf[...].reshape(-1, tbuf.shape[2]), wbuf[...], preferred_element_type=F32) + bbuf[...]
    out[...] = y.astype(BF).reshape(out.shape)


def far_proj_kernel(tok, w, bias, far, wbuf, bbuf, tbuf, sems, *, axis):
    far_at = jnp.where(near_is_top(axis), tok.shape[0] - HALO, 0)
    copies = [
        pltpu.make_async_copy(w, wbuf, sems.at[0]),
        pltpu.make_async_copy(bias, bbuf, sems.at[1]),
        pltpu.make_async_copy(tok.at[pl.ds(far_at, HALO)], tbuf, sems.at[2]),
    ]
    for c in copies:
        c.start()
    for c in copies:
        c.wait()
    project(tbuf, wbuf, bbuf, far)


def near_proj_kernel(wbuf, bbuf, far, tok, feature, near, tbuf, rest, sem, *, axis):
    flip = near_is_top(axis)
    count = rest.shape[0]
    copy = pltpu.make_async_copy(tok.at[pl.ds(jnp.where(flip, 0, HALO), count)], tbuf, sem)
    copy.start()
    copy.wait()
    project(tbuf, wbuf, bbuf, rest)
    feature[pl.ds(jnp.where(flip, HALO, 2 * HALO), count)] = rest[...]
    feature[pl.ds(jnp.where(flip, HALO + count, HALO), HALO)] = far[...]
    near[...] = rest[pl.ds(jnp.where(flip, 0, count - HALO), HALO)]


def relu_row(x):
    return jnp.maximum(x.astype(F32), 0.0)


def pick(cond, a, b):
    return jnp.where(cond, a.astype(F32), b.astype(F32))


def conv0_inner_kernel(feature, cw, c_ref, part, w0, w_next, a3, sems, *, strip):
    waits = [[pltpu.make_async_copy(cw.at[0, dy], w0.at[dy], sems.at[dy])] for dy in range(3)]
    late = pltpu.make_async_copy(cw.at[1, 0], w_next, sems.at[3])
    for copy in (*waits[0], *waits[1], *waits[2], late):
        copy.start()

    def row_at(i):
        return relu_row(feature[HALO + i])

    w_parts = [w0.at[dy] for dy in range(3)]
    part[0], part[1] = run_conv(row_at, strip, a3, w_parts, waits, c_ref, 4, 1, strip, tile=SHAPES["inner"])
    late.wait()


def conv0_edge(got, feature, w0, part, c_ref, a3, upper, strip):
    feature[pl.ds(jnp.where(upper, 0, strip + HALO), HALO)] = got
    base = jnp.where(upper, 0, strip)

    def row_at(i):
        return relu_row(feature[base + i])

    w_parts = [w0.at[dy] for dy in range(3)]
    run_conv(row_at, HALO + 2, a3, w_parts, [[]] * 3, c_ref, base + 2, strip, strip, tile=SHAPES["outer"])
    row = c_ref[jnp.where(upper, 3, strip + 2)]
    return part[0] + fold8(row), part[1] + fold8(row * row)


def conv0_near_kernel(got, w0, part_in, c_in, feature_in, c_ref, part, feature, a3, *, strip, axis):
    part[0], part[1] = conv0_edge(got[...], feature, w0, part_in, c_ref, a3, near_is_top(axis), strip)


def conv0_far_kernel(got, w0, part, c_in, feature_in, c_ref, st, feature, a3, *, strip, axis):
    r = lax.axis_index(axis)
    exists = jnp.logical_and(r > 0, r < lax.axis_size(axis) - 1).astype(F32)
    rows = (got[...].astype(F32) * exists).astype(BF)
    upper = jnp.logical_not(near_is_top(axis))
    write_stats(st, *conv0_edge(rows, feature, w0, part, c_ref, a3, upper, strip))


def weight_copies(cw, k, wbuf, w_next, sems):
    waits = [[]] + [[pltpu.make_async_copy(cw.at[k, dy], wbuf.at[dy - 1], sems.at[dy - 1])] for dy in (1, 2)]
    late = []
    if w_next is not None:
        late.append(pltpu.make_async_copy(cw.at[k + 1, 0], w_next, sems.at[2]))
    for c in waits[1]:
        c.start()
    for c in waits[2] + late:
        c.start()
    return waits, late


def hidden_conv_kernel(
    c_in, stats, gain, shift, w_first, cw, c_ref, st, *rest, k, lo, n_in, at, strip, total, axis
):
    *more, a3, wbuf, sems = rest
    waits, late = weight_copies(cw, k + 1, wbuf, more[0] if more else None, sems)
    mean, scale, bias = norm_terms(stats, gain, shift, k, total)

    def row_at(i):
        x = jnp.maximum((c_in[at + i] - mean) * scale + bias, 0.0)
        return masked(x, inside(lo + i, strip, axis))

    w_parts = [w_first, wbuf.at[0], wbuf.at[1]]
    write_stats(st, *run_conv(row_at, n_in, a3, w_parts, waits, c_ref, at, lo + 1, strip, tile=SHAPES[k]))
    if more:
        flip = near_is_top(axis)
        far, near = more[1:]
        far[...] = c_ref[pl.ds(jnp.where(flip, at + strip - HALO, at), HALO)].astype(BF)
        near[...] = c_ref[pl.ds(jnp.where(flip, at, at + strip - HALO), HALO)].astype(BF)
    for c in late:
        c.wait()


def joined_conv_kernel(
    c_in, stats, gain, shift, w_first, feature, got_far, got_near, cw, c_ref, st, w_next, joined, a3, wbuf, sems,
    *, k, lo, n_in, at, strip, total, axis
):
    waits, late = weight_copies(cw, k + 1, wbuf, w_next, sems)
    mean, scale, bias = norm_terms(stats, gain, shift, k, total)
    flip = near_is_top(axis)

    def conv_row(i):
        if i < HALO:
            return pick(flip, got_near[i], got_far[i])
        if i < HALO + strip:
            return c_in[i]
        return pick(flip, got_far[i - HALO - strip], got_near[i - HALO - strip])

    def row_at(i):
        y = (feature[i].astype(F32) + ((conv_row(i) - mean) * scale + bias)).astype(BF)
        joined[i] = y
        return masked(relu_row(y), inside(lo + i, strip, axis))

    w_parts = [w_first, wbuf.at[0], wbuf.at[1]]
    write_stats(st, *run_conv(row_at, n_in, a3, w_parts, waits, c_ref, at, lo + 1, strip, tile=SHAPES[k]))
    for c in late:
        c.wait()


def final_kernel(joined, c_in, stats, gain, shift, out, rows, sems, *, k, total):
    mean, scale, bias = norm_terms(stats, gain, shift, k, total)
    copies = []
    for i in range(0, rows.shape[0], 2):
        for j in (i, i + 1):
            rows[j] = (joined[j + 2].astype(F32) + ((c_in[j] - mean) * scale + bias)).astype(BF)
        copies.append(pltpu.make_async_copy(rows.at[i : i + 2], out.at[i : i + 2], sems.at[i // 2]))
        copies[-1].start()
    for c in copies:
        c.wait()


def sent_to_all(value, axis):
    return lax.all_to_all(value, axis, 0, 0, tiled=True)


def reduce_all(partial):
    near = sent_to_all(partial, "row").sum(axis=0)
    far = lax.axis_size("img")
    return sent_to_all(jnp.broadcast_to(near[None], (far, *near.shape)), "img")


def swapped(value, firsts):
    pairs = [(i, (i + 1) % lax.axis_size("row")) for i in firsts]
    return lax.ppermute(value, "row", pairs + [(j, i) for i, j in pairs])


def on_device(tokens, proj_weight, proj_bias, conv_weight, bn_gain, bn_bias):
    imgs, strip, cols, embed = tokens.shape
    ch = proj_weight.shape[1]
    nrow = lax.axis_size("row")
    total = float(lax.axis_size("img") * nrow * imgs * strip * cols)
    weights = in_hbm(conv_weight)
    norm_args = (bn_gain, bn_bias)

    half = sds((HALO, cols, ch), BF)
    w_third = sds((3, ch, ch), BF)
    token_rows = in_hbm(tokens[0])
    far, pw, pb = pl.pallas_call(
        functools.partial(far_proj_kernel, axis="row"),
        out_shape=(half, sds((embed, ch), BF), sds((1, ch), F32)),
        in_specs=[HBM] * 3,
        out_specs=(VM,) * 3,
        scratch_shapes=[pltpu.VMEM((HALO, cols, embed), BF), pltpu.SemaphoreType.DMA((3,))],
        compiler_params=PARAMS,
    )(token_rows, in_hbm(proj_weight), in_hbm(proj_bias[None]))
    far_pairs, near_pairs = range(1, nrow, 2), range(0, nrow - 1, 2)
    context = sds((strip + 2 * HALO, cols, ch), BF)
    got_far = swapped(far, far_pairs)
    near_call = pl.pallas_call(
        functools.partial(near_proj_kernel, axis="row"),
        out_shape=(context, half),
        in_specs=[VM, VM, VM, HBM],
        out_specs=(VM, VM),
        scratch_shapes=[
            pltpu.VMEM((strip - HALO, cols, embed), BF),
            pltpu.VMEM((strip - HALO, cols, ch), BF),
            pltpu.SemaphoreType.DMA(()),
        ],
        compiler_params=PARAMS,
        cost_estimate=pl.CostEstimate(
            flops=2 * embed * ch * cols * (strip - HALO), transcendentals=0, bytes_accessed=2 * strip * cols * embed
        ),
    )
    feature, near = near_call(in_vmem(pw), in_vmem(pb), in_vmem(far), token_rows)
    got_near = swapped(near, near_pairs)

    field = sds((strip + 4, cols, ch), F32)
    stat = sds((nrow, 1, 2 * ch), F32)

    def rows_scratch(rows):
        return pltpu.VMEM((rows, cols, 3 * ch), BF)

    sums = sds((2, 8, ch), F32)

    def conv_flops(rows):
        return pl.CostEstimate(
            flops=2 * 9 * ch * ch * cols * rows, transcendentals=0, bytes_accessed=9 * ch * ch * 2
        )

    c, part, w0, w_next = pl.pallas_call(
        functools.partial(conv0_inner_kernel, strip=strip),
        out_shape=(field, sums, sds((3, 3, ch, ch), BF), w_third),
        in_specs=[VM, HBM],
        out_specs=(VM,) * 4,
        scratch_shapes=[rows_scratch(strip), pltpu.SemaphoreType.DMA((4,))],
        compiler_params=PARAMS,
        cost_estimate=conv_flops(strip - 2),
    )(in_vmem(feature), weights)

    def edge(kernel, got, part, c, feature, out):
        return pl.pallas_call(
            functools.partial(kernel, strip=strip, axis="row"),
            out_shape=(field, out, context),
            in_specs=[VM] * 5,
            out_specs=(VM,) * 3,
            input_output_aliases={3: 0, 4: 2},
            scratch_shapes=[rows_scratch(HALO + 2)],
            compiler_params=PARAMS,
            cost_estimate=conv_flops(HALO),
        )(*map(in_vmem, (got, w0, part, c, feature)))

    c, part, feature = edge(conv0_near_kernel, got_near, part, c, feature, sums)
    c, st, feature = edge(conv0_far_kernel, got_far, part, c, feature, stat)

    def call(kernel, extra_in, extra_out, n_in, aliases, **kw):
        args = (in_vmem(c), in_vmem(st), *norm_args, *map(in_vmem, extra_in))
        return pl.pallas_call(
            functools.partial(kernel, n_in=n_in, strip=strip, total=total, axis="row", **kw),
            out_shape=(field, stat, *extra_out),
            in_specs=[VM] * len(args) + [HBM],
            out_specs=(VM,) * (2 + len(extra_out)),
            input_output_aliases={0: 0, **aliases},
            scratch_shapes=[
                rows_scratch(n_in),
                pltpu.VMEM((2, 3, ch, ch), BF),
                pltpu.SemaphoreType.DMA((3,)),
            ],
            compiler_params=PARAMS,
        )(*args, weights)

    edge_rows = pltpu.VMEM((HALO, cols, ch), BF)
    st = reduce_all(st)
    c, st, w_next, far, near = call(
        hidden_conv_kernel, (w_next,), (w_third, edge_rows, edge_rows), strip + 2, {}, k=0, lo=-1, at=2
    )
    got_far = swapped(far, far_pairs)
    got_near = swapped(near, near_pairs)
    st = reduce_all(st)
    c, st, w_next, joined = call(
        joined_conv_kernel, (w_next, feature, got_far, got_near), (w_third, context), strip + 4, {5: 3},
        k=1, lo=-2, at=0,
    )
    st = reduce_all(st)
    c, st = call(hidden_conv_kernel, (w_next,), (), strip + 2, {}, k=2, lo=-1, at=0)
    st = reduce_all(st)
    out = pl.pallas_call(
        functools.partial(final_kernel, k=3, total=total),
        out_shape=sds((strip, cols, ch), BF),
        in_specs=[VM] * 5,
        out_specs=HBM,
        scratch_shapes=[pltpu.VMEM((strip, cols, ch), BF), pltpu.SemaphoreType.DMA((strip // 2,))],
        compiler_params=PARAMS,
    )(in_vmem(joined), in_vmem(c), in_vmem(st), *norm_args)
    return out[None]


def solution(mesh):
    placed = (P("img", "row", None, None), P(), P(), P(), P(), P())
    return jax.shard_map(
        on_device, mesh=mesh, in_specs=placed, out_specs=P("img", "row", None, None), check_vma=False
    )
```

```python
import functools

import jax
import jax.numpy as jnp
from jax import lax
from jax.experimental import pallas as pl
from jax.experimental.pallas import tpu as pltpu
from jax.sharding import PartitionSpec as P


EPS = 1e-05
HALO = 4
SHAPES = {'inner': (3, 0), 'outer': (2, 0), 0: (2, 0), 1: (5, 0), 2: (2, 0)}
VM = pl.BlockSpec(memory_space=pltpu.VMEM)
HBM = pl.BlockSpec(memory_space=pltpu.HBM)
BF = jnp.bfloat16
F32 = jnp.float32
PARAMS = pltpu.CompilerParams(vmem_limit_bytes=24 << 20)
LP_PARAMS = pltpu.CompilerParams(vmem_limit_bytes=24 << 20)


def sds(shape, dtype):
    return jax.ShapeDtypeStruct(shape, dtype)


def in_hbm(x):
    return pltpu.with_memory_space_constraint(x, pltpu.HBM)


def in_vmem(x):
    return pltpu.with_memory_space_constraint(x, pltpu.VMEM)


def put_row(a3, row, x):
    cols, ch = x.shape
    col = lax.broadcasted_iota(jnp.int32, x.shape, 0)
    a3[row, :, ch : 2 * ch] = x.astype(BF)
    a3[row, :, 0:ch] = jnp.where(col == 0, 0.0, pltpu.roll(x, 1, 0)).astype(BF)
    a3[row, :, 2 * ch :] = jnp.where(col == cols - 1, 0.0, pltpu.roll(x, cols - 1, 0)).astype(BF)


def fold8(x):
    return x.reshape(-1, 8, x.shape[-1]).sum(axis=0)


def norm_terms(stats_ref, gain_ref, bias_ref, k, total):
    s = jnp.sum(stats_ref[...], axis=0)
    ch = s.shape[-1] // 2
    mean = s[:, :ch] / total
    spread = jnp.maximum(s[:, ch:] / total - mean * mean, 0.0)
    return mean, lax.rsqrt(spread + EPS) * gain_ref[k : k + 1, :], bias_ref[k : k + 1, :]


def write_stats(out_ref, sums, squares):
    both = jnp.concatenate(
        [jnp.sum(sums, axis=0, keepdims=True), jnp.sum(squares, axis=0, keepdims=True)], axis=1
    )
    out_ref[...] = jnp.broadcast_to(both[None], out_ref.shape)


def inside(local_row, strip, axis):
    if 0 <= local_row < strip:
        return None
    r = lax.axis_index(axis)
    edge = r > 0 if local_row < 0 else r < lax.axis_size(axis) - 1
    return edge.astype(F32)


def masked(x, m):
    return x if m is None else x * m


def run_conv(row_at, n_in, a3, w_parts, waits, c_ref, at, lo, strip, sums=None, squares=None, tile=(2, 0), refill=None):
    cols, ch = c_ref.shape[1:]
    n_out = n_in - 2
    step, ahead = tile
    filled = 0
    for dy in range(3):
        for copy in waits[dy]:
            copy.wait()
        w = w_parts[dy][...].reshape(3 * ch, ch)
        for done in range(0, n_out, step):
            rows = min(step, n_out - done)
            while filled < min(n_in, done + rows + dy + ahead):
                put_row(a3, filled, row_at(filled))
                filled += 1
            lhs = a3[done + dy : done + dy + rows].reshape(rows * cols, 3 * ch)
            acc = jnp.dot(lhs, w, preferred_element_type=F32)
            into = pl.ds(at + done, rows)
            if dy:
                acc = acc + c_ref[into].reshape(rows * cols, ch)
            c_ref[into] = acc.reshape(rows, cols, ch)
            own_from = max(0, -(lo + done))
            own_to = min(rows, strip - (lo + done))
            if dy == 2 and own_to > own_from:
                own = acc[own_from * cols : own_to * cols]
                s, q = fold8(own), fold8(own * own)
                sums = s if sums is None else sums + s
                squares = q if squares is None else squares + q
        if dy == 0 and refill is not None:
            refill.start()
    return sums, squares


def near_is_top(axis):
    return lax.axis_index(axis) % 2 == 1


def project(tbuf, wbuf, bbuf, out):
    y = jnp.dot(tbuf[...].reshape(-1, tbuf.shape[2]), wbuf[...], preferred_element_type=F32) + bbuf[...]
    out[...] = y.astype(BF).reshape(out.shape)


def far_proj_kernel(tok, w, bias, far, wbuf, bbuf, tbuf, sems, *, axis):
    far_at = jnp.where(near_is_top(axis), HALO, 0)
    copies = [
        pltpu.make_async_copy(w, wbuf, sems.at[0]),
        pltpu.make_async_copy(bias, bbuf, sems.at[1]),
        pltpu.make_async_copy(tok.at[pl.ds(far_at, HALO)], tbuf, sems.at[2]),
    ]
    for c in copies:
        c.start()
    for c in copies:
        c.wait()
    project(tbuf, wbuf, bbuf, far)


def near_proj_kernel(wbuf, bbuf, tok, near, tbuf, sem, *, axis):
    copy = pltpu.make_async_copy(tok.at[pl.ds(jnp.where(near_is_top(axis), 0, HALO), HALO)], tbuf, sem)
    copy.start()
    copy.wait()
    project(tbuf, wbuf, bbuf, near)


def relu_row(x):
    return jnp.maximum(x.astype(F32), 0.0)


def pick(cond, a, b):
    return jnp.where(cond, a.astype(F32), b.astype(F32))


def conv0_inner_kernel(far, near, cw, c_ref, part, w0, w_first, w_second, a3, sems, *, strip, axis):
    waits = [[pltpu.make_async_copy(cw.at[0, dy], w0.at[dy], sems.at[dy])] for dy in range(3)]
    late = [pltpu.make_async_copy(cw.at[1, dy], (w_first, w_second)[dy], sems.at[3 + dy]) for dy in range(2)]
    for copy in (*waits[0], *waits[1], *waits[2], *late):
        copy.start()
    flip = near_is_top(axis)

    def row_at(i):
        j = i % HALO
        return relu_row(pick(flip, near[j], far[j]) if i < HALO else pick(flip, far[j], near[j]))

    w_parts = [w0.at[dy] for dy in range(3)]
    part[0], part[1] = run_conv(row_at, strip, a3, w_parts, waits, c_ref, HALO, 1, strip, tile=SHAPES["inner"])
    for copy in late:
        copy.wait()


def conv0_edge(got, own, w0, part, c_ref, a3, upper, strip, exists=None):
    def theirs(i):
        return got[i] if exists is None else got[i].astype(F32) * exists

    def row_at(i):
        above = theirs(i) if i < HALO else own[i - HALO]
        below = own[i + HALO - 2] if i < 2 else theirs(i - 2)
        return relu_row(pick(upper, above, below))

    w_parts = [w0.at[dy] for dy in range(3)]
    at = jnp.where(upper, 0, strip + HALO - 2)
    run_conv(row_at, HALO + 2, a3, w_parts, [[]] * 3, c_ref, at, strip, strip, tile=SHAPES["outer"])
    row = c_ref[jnp.where(upper, HALO - 1, strip + HALO - 2)]
    return part[0] + fold8(row), part[1] + fold8(row * row)


def conv0_near_kernel(got, far, near, w0, part_in, c_in, c_ref, part, feature, a3, *, strip, axis):
    flip = near_is_top(axis)
    part[0], part[1] = conv0_edge(got, near, w0, part_in, c_ref, a3, flip, strip)
    near_at = jnp.where(flip, 0, HALO)
    feature[pl.ds(2 + near_at, HALO)] = near[...]
    feature[pl.ds(2 + HALO - near_at, HALO)] = far[...]
    feature[pl.ds(jnp.where(flip, 0, strip + 2), 2)] = got[pl.ds(jnp.where(flip, HALO - 2, 0), 2)]


def conv0_far_kernel(got, far, w0, part, c_in, feature_in, c_ref, st, feature, a3, *, strip, axis):
    flip = near_is_top(axis)
    upper = jnp.logical_not(flip)
    r = lax.axis_index(axis)
    exists = jnp.logical_and(r > 0, r < lax.axis_size(axis) - 1).astype(F32)
    sums, squares = conv0_edge(got, far, w0, part, c_ref, a3, upper, strip, exists)
    write_stats(st, sums, squares)
    feature[pl.ds(jnp.where(flip, strip + 2, 0), 2)] = got[pl.ds(jnp.where(flip, 0, HALO - 2), 2)]


def weight_copies(cw, k, parts, first, sems):
    waits = [[] for _ in parts]
    for dy in range(first, len(parts)):
        waits[dy].append(pltpu.make_async_copy(cw.at[k, dy], parts[dy], sems.at[dy - 1]))
        waits[dy][0].start()
    return waits


def hidden_conv_kernel(
    c_in, stats, gain, shift, w_first, w_second, cw, c_ref, st, *rest, k, lo, n_in, strip, total, axis
):
    *w_next, a3, wbuf, sems = rest
    refill = None
    if w_next:
        (w_first,) = w_next
        refill = pltpu.make_async_copy(cw.at[k + 2, 0], w_first, sems.at[2])
    w_parts = [w_first, w_second, wbuf.at[0]]
    waits = weight_copies(cw, k + 1, w_parts, 2, sems)
    mean, scale, bias = norm_terms(stats, gain, shift, k, total)

    def row_at(i):
        x = jnp.maximum((c_in[i] - mean) * scale + bias, 0.0)
        return masked(x, inside(lo + i, strip, axis))

    write_stats(
        st, *run_conv(row_at, n_in, a3, w_parts, waits, c_ref, 0, lo + 1, strip, tile=SHAPES[k], refill=refill)
    )
    if refill is not None:
        refill.wait()


def joined_conv_kernel(
    c_in, stats, gain, shift, w_in, feature, cw, c_ref, st, w_first, w_second, joined, a3, wbuf, sems,
    *, k, lo, n_in, strip, total, axis
):
    w_parts = [w_first, wbuf.at[0], wbuf.at[1]]
    waits = weight_copies(cw, k + 1, w_parts, 1, sems)
    late = pltpu.make_async_copy(cw.at[k + 2, 1], w_second, sems.at[3])
    late.start()
    refill = pltpu.make_async_copy(cw.at[k + 2, 0], w_first, sems.at[2])
    mean, scale, bias = norm_terms(stats, gain, shift, k, total)

    def row_at(i):
        y = (feature[i].astype(F32) + ((c_in[i] - mean) * scale + bias)).astype(BF)
        joined[i] = y
        return masked(relu_row(y), inside(lo + i, strip, axis))

    write_stats(
        st, *run_conv(row_at, n_in, a3, w_parts, waits, c_ref, 0, lo + 1, strip, tile=SHAPES[k], refill=refill)
    )
    late.wait()
    refill.wait()


def final_kernel(joined, c_in, stats, gain, shift, out, rows, sems, *, k, total):
    mean, scale, bias = norm_terms(stats, gain, shift, k, total)
    copies = []
    for i in range(0, rows.shape[0], 2):
        for j in (i, i + 1):
            rows[j] = (joined[j + 2].astype(F32) + ((c_in[j] - mean) * scale + bias)).astype(BF)
        copies.append(pltpu.make_async_copy(rows.at[i : i + 2], out.at[i : i + 2], sems.at[i // 2]))
        copies[-1].start()
    for c in copies:
        c.wait()


def sent_to_all(value, axis):
    return lax.all_to_all(value, axis, 0, 0, tiled=True)


def reduce_all(partial):
    near = sent_to_all(partial, "row").sum(axis=0)
    far = lax.axis_size("img")
    return sent_to_all(jnp.broadcast_to(near[None], (far, *near.shape)), "img")


def swapped(value, firsts):
    pairs = [(i, (i + 1) % lax.axis_size("row")) for i in firsts]
    return lax.ppermute(value, "row", pairs + [(j, i) for i, j in pairs])


def on_device(tokens, proj_weight, proj_bias, conv_weight, bn_gain, bn_bias):
    imgs, strip, cols, embed = tokens.shape
    ch = proj_weight.shape[1]
    nrow = lax.axis_size("row")
    total = float(lax.axis_size("img") * nrow * imgs * strip * cols)
    weights = in_hbm(conv_weight)
    norm_args = (bn_gain, bn_bias)

    half = sds((HALO, cols, ch), BF)
    w_third = sds((3, ch, ch), BF)
    token_rows = in_hbm(tokens[0])
    far, pw, pb = pl.pallas_call(
        functools.partial(far_proj_kernel, axis="row"),
        out_shape=(half, sds((embed, ch), BF), sds((1, ch), F32)),
        in_specs=[HBM] * 3,
        out_specs=(VM,) * 3,
        scratch_shapes=[pltpu.VMEM((HALO, cols, embed), BF), pltpu.SemaphoreType.DMA((3,))],
        compiler_params=PARAMS,
    )(token_rows, in_hbm(proj_weight), in_hbm(proj_bias[None]))
    got_far = swapped(far, range(1, nrow, 2))
    near_call = pl.pallas_call(
        functools.partial(near_proj_kernel, axis="row"),
        out_shape=half,
        in_specs=[VM, VM, HBM],
        out_specs=VM,
        scratch_shapes=[pltpu.VMEM((HALO, cols, embed), BF), pltpu.SemaphoreType.DMA(())],
        compiler_params=PARAMS,
        cost_estimate=pl.CostEstimate(
            flops=2 * embed * ch * cols * HALO, transcendentals=0, bytes_accessed=2 * HALO * cols * embed
        ),
    )
    near = near_call(in_vmem(pw), in_vmem(pb), token_rows)
    got_near = swapped(near, range(0, nrow - 1, 2))
    far, near, got_far, got_near = map(in_vmem, (far, near, got_far, got_near))

    field = sds((strip + 2 * HALO - 2, cols, ch), F32)
    stat = sds((nrow, 1, 2 * ch), F32)
    context = sds((strip + 4, cols, ch), BF)

    def rows_scratch(rows):
        return pltpu.VMEM((rows, cols, 3 * ch), BF)

    sums = sds((2, 8, ch), F32)

    def conv_flops(rows):
        return pl.CostEstimate(
            flops=2 * 9 * ch * ch * cols * rows, transcendentals=0, bytes_accessed=9 * ch * ch * 2
        )

    c, part, w0, w_first, w_second = pl.pallas_call(
        functools.partial(conv0_inner_kernel, strip=strip, axis="row"),
        out_shape=(field, sums, sds((3, 3, ch, ch), BF), w_third, w_third),
        in_specs=[VM, VM, HBM],
        out_specs=(VM,) * 5,
        scratch_shapes=[rows_scratch(strip), pltpu.SemaphoreType.DMA((5,))],
        compiler_params=PARAMS,
        cost_estimate=conv_flops(strip - 2),
    )(far, near, weights)
    w0 = in_vmem(w0)
    c, part, feature = pl.pallas_call(
        functools.partial(conv0_near_kernel, strip=strip, axis="row"),
        out_shape=(field, sums, context),
        in_specs=[VM] * 6,
        out_specs=(VM,) * 3,
        input_output_aliases={5: 0},
        scratch_shapes=[rows_scratch(HALO + 2)],
        compiler_params=PARAMS,
        cost_estimate=conv_flops(HALO),
    )(got_near, far, near, w0, in_vmem(part), in_vmem(c))
    c, st, feature = pl.pallas_call(
        functools.partial(conv0_far_kernel, strip=strip, axis="row"),
        out_shape=(field, stat, context),
        in_specs=[VM] * 6,
        out_specs=(VM,) * 3,
        input_output_aliases={4: 0, 5: 2},
        scratch_shapes=[rows_scratch(HALO + 2)],
        compiler_params=PARAMS,
        cost_estimate=conv_flops(HALO),
    )(got_far, far, w0, in_vmem(part), in_vmem(c), in_vmem(feature))

    def call(kernel, extra_in, extra_out, n_in, aliases, **kw):
        args = (in_vmem(c), in_vmem(st), *norm_args, *map(in_vmem, extra_in))
        return pl.pallas_call(
            functools.partial(kernel, n_in=n_in, strip=strip, total=total, axis="row", **kw),
            out_shape=(field, stat, *extra_out),
            in_specs=[VM] * len(args) + [HBM],
            out_specs=(VM,) * (2 + len(extra_out)),
            input_output_aliases={0: 0, **aliases},
            scratch_shapes=[
                rows_scratch(n_in),
                pltpu.VMEM((2, 3, ch, ch), BF),
                pltpu.SemaphoreType.DMA((4,)),
            ],
            compiler_params=LP_PARAMS if kernel is joined_conv_kernel else PARAMS,
        )(*args, weights)

    st = reduce_all(st)
    c, st, w_first = call(
        hidden_conv_kernel, (w_first, w_second), (w_third,), strip + 6, {4: 2}, k=0, lo=-3
    )
    st = reduce_all(st)
    c, st, w_first, w_second, joined = call(
        joined_conv_kernel, (w_first, feature), (w_third, w_third, context), strip + 4, {4: 2, 5: 4}, k=1, lo=-2
    )
    st = reduce_all(st)
    c, st = call(hidden_conv_kernel, (w_first, w_second), (), strip + 2, {}, k=2, lo=-1)
    st = reduce_all(st)
    out = pl.pallas_call(
        functools.partial(final_kernel, k=3, total=total),
        out_shape=sds((strip, cols, ch), BF),
        in_specs=[VM] * 5,
        out_specs=HBM,
        scratch_shapes=[pltpu.VMEM((strip, cols, ch), BF), pltpu.SemaphoreType.DMA((strip // 2,))],
        compiler_params=PARAMS,
    )(in_vmem(joined), in_vmem(c), in_vmem(st), *norm_args)
    return out[None]


def solution(mesh):
    placed = (P("img", "row", None, None), P(), P(), P(), P(), P())
    return jax.shard_map(
        on_device, mesh=mesh, in_specs=placed, out_specs=P("img", "row", None, None), check_vma=False
    )
```

```python
import functools

import jax
import jax.numpy as jnp
from jax import lax
from jax.experimental import pallas as pl
from jax.experimental.pallas import tpu as pltpu
from jax.sharding import PartitionSpec as P


EPS = 1e-05
HALO = 4
SHAPES = {'inner': (3, 0), 'outer': (2, 0), 0: (2, 0), 1: (5, 0), 2: (2, 0)}
VM = pl.BlockSpec(memory_space=pltpu.VMEM)
HBM = pl.BlockSpec(memory_space=pltpu.HBM)
BF = jnp.bfloat16
F32 = jnp.float32
PARAMS = pltpu.CompilerParams(vmem_limit_bytes=24 << 20)


def sds(shape, dtype):
    return jax.ShapeDtypeStruct(shape, dtype)


def in_hbm(x):
    return pltpu.with_memory_space_constraint(x, pltpu.HBM)


def in_vmem(x):
    return pltpu.with_memory_space_constraint(x, pltpu.VMEM)


def put_row(a3, row, x):
    cols, ch = x.shape
    col = lax.broadcasted_iota(jnp.int32, x.shape, 0)
    a3[row, :, ch : 2 * ch] = x.astype(BF)
    a3[row, :, 0:ch] = jnp.where(col == 0, 0.0, pltpu.roll(x, 1, 0)).astype(BF)
    a3[row, :, 2 * ch :] = jnp.where(col == cols - 1, 0.0, pltpu.roll(x, cols - 1, 0)).astype(BF)


def fold8(x):
    return x.reshape(-1, 8, x.shape[-1]).sum(axis=0)


def norm_terms(stats_ref, gain_ref, bias_ref, k, total):
    s = jnp.sum(stats_ref[...], axis=0)
    ch = s.shape[-1] // 2
    mean = s[:, :ch] / total
    spread = jnp.maximum(s[:, ch:] / total - mean * mean, 0.0)
    return mean, lax.rsqrt(spread + EPS) * gain_ref[k : k + 1, :], bias_ref[k : k + 1, :]


def write_stats(out_ref, sums, squares):
    both = jnp.concatenate(
        [jnp.sum(sums, axis=0, keepdims=True), jnp.sum(squares, axis=0, keepdims=True)], axis=1
    )
    out_ref[...] = jnp.broadcast_to(both[None], out_ref.shape)


def inside(local_row, strip, axis):
    if 0 <= local_row < strip:
        return None
    r = lax.axis_index(axis)
    edge = r > 0 if local_row < 0 else r < lax.axis_size(axis) - 1
    return edge.astype(F32)


def masked(x, m):
    return x if m is None else x * m


def run_conv(row_at, n_in, a3, w_parts, waits, c_ref, at, lo, strip, sums=None, squares=None, tile=(2, 0), refill=None):
    cols, ch = c_ref.shape[1:]
    n_out = n_in - 2
    step, ahead = tile
    filled = 0
    for dy in range(3):
        for copy in waits[dy]:
            copy.wait()
        w = w_parts[dy][...].reshape(3 * ch, ch)
        for done in range(0, n_out, step):
            rows = min(step, n_out - done)
            while filled < min(n_in, done + rows + dy + ahead):
                put_row(a3, filled, row_at(filled))
                filled += 1
            lhs = a3[done + dy : done + dy + rows].reshape(rows * cols, 3 * ch)
            acc = jnp.dot(lhs, w, preferred_element_type=F32)
            into = pl.ds(at + done, rows)
            if dy:
                acc = acc + c_ref[into].reshape(rows * cols, ch)
            c_ref[into] = acc.reshape(rows, cols, ch)
            own_from = max(0, -(lo + done))
            own_to = min(rows, strip - (lo + done))
            if dy == 2 and own_to > own_from:
                own = acc[own_from * cols : own_to * cols]
                s, q = fold8(own), fold8(own * own)
                sums = s if sums is None else sums + s
                squares = q if squares is None else squares + q
        if dy == 0 and refill is not None:
            for copy in refill:
                copy.start()
    return sums, squares


def near_is_top(axis):
    return lax.axis_index(axis) % 2 == 1


def project(tbuf, wbuf, bbuf, out):
    y = jnp.dot(tbuf[...].reshape(-1, tbuf.shape[2]), wbuf[...], preferred_element_type=F32) + bbuf[...]
    out[...] = y.astype(BF).reshape(out.shape)


def far_proj_kernel(tok, w, bias, far, wbuf, bbuf, tbuf, sems, *, axis):
    far_at = jnp.where(near_is_top(axis), HALO, 0)
    copies = [
        pltpu.make_async_copy(w, wbuf, sems.at[0]),
        pltpu.make_async_copy(bias, bbuf, sems.at[1]),
        pltpu.make_async_copy(tok.at[pl.ds(far_at, HALO)], tbuf, sems.at[2]),
    ]
    for c in copies:
        c.start()
    for c in copies:
        c.wait()
    project(tbuf, wbuf, bbuf, far)


def near_proj_kernel(wbuf, bbuf, tok, near, tbuf, sem, *, axis):
    copy = pltpu.make_async_copy(tok.at[pl.ds(jnp.where(near_is_top(axis), 0, HALO), HALO)], tbuf, sem)
    copy.start()
    copy.wait()
    project(tbuf, wbuf, bbuf, near)


def relu_row(x):
    return jnp.maximum(x.astype(F32), 0.0)


def pick(cond, a, b):
    return jnp.where(cond, a.astype(F32), b.astype(F32))


def conv0_inner_kernel(far, near, cw, c_ref, part, w0, w_first, w_second, a3, sems, *, strip, axis):
    waits = [[pltpu.make_async_copy(cw.at[0, dy], w0.at[dy], sems.at[dy])] for dy in range(3)]
    late = [pltpu.make_async_copy(cw.at[1, dy], (w_first, w_second)[dy], sems.at[3 + dy]) for dy in range(2)]
    for copy in (*waits[0], *waits[1], *waits[2], *late):
        copy.start()
    flip = near_is_top(axis)

    def row_at(i):
        j = i % HALO
        return relu_row(pick(flip, near[j], far[j]) if i < HALO else pick(flip, far[j], near[j]))

    w_parts = [w0.at[dy] for dy in range(3)]
    part[0], part[1] = run_conv(row_at, strip, a3, w_parts, waits, c_ref, HALO, 1, strip, tile=SHAPES["inner"])
    for copy in late:
        copy.wait()


def conv0_edge(got, own, w0, part, c_ref, a3, upper, strip, exists=None):
    def theirs(i):
        return got[i] if exists is None else got[i].astype(F32) * exists

    def row_at(i):
        above = theirs(i) if i < HALO else own[i - HALO]
        below = own[i + HALO - 2] if i < 2 else theirs(i - 2)
        return relu_row(pick(upper, above, below))

    w_parts = [w0.at[dy] for dy in range(3)]
    at = jnp.where(upper, 0, strip + HALO - 2)
    run_conv(row_at, HALO + 2, a3, w_parts, [[]] * 3, c_ref, at, strip, strip, tile=SHAPES["outer"])
    row = c_ref[jnp.where(upper, HALO - 1, strip + HALO - 2)]
    return part[0] + fold8(row), part[1] + fold8(row * row)


def conv0_near_kernel(got, far, near, w0, part_in, c_in, c_ref, part, feature, a3, *, strip, axis):
    flip = near_is_top(axis)
    part[0], part[1] = conv0_edge(got, near, w0, part_in, c_ref, a3, flip, strip)
    near_at = jnp.where(flip, 0, HALO)
    feature[pl.ds(2 + near_at, HALO)] = near[...]
    feature[pl.ds(2 + HALO - near_at, HALO)] = far[...]
    feature[pl.ds(jnp.where(flip, 0, strip + 2), 2)] = got[pl.ds(jnp.where(flip, HALO - 2, 0), 2)]


def conv0_far_kernel(got, far, w0, part, c_in, feature_in, c_ref, st, feature, a3, *, strip, axis):
    flip = near_is_top(axis)
    upper = jnp.logical_not(flip)
    r = lax.axis_index(axis)
    exists = jnp.logical_and(r > 0, r < lax.axis_size(axis) - 1).astype(F32)
    sums, squares = conv0_edge(got, far, w0, part, c_ref, a3, upper, strip, exists)
    write_stats(st, sums, squares)
    feature[pl.ds(jnp.where(flip, strip + 2, 0), 2)] = got[pl.ds(jnp.where(flip, 0, HALO - 2), 2)]


def weight_copies(cw, k, parts, first, sems):
    waits = [[] for _ in parts]
    for dy in range(first, len(parts)):
        waits[dy].append(pltpu.make_async_copy(cw.at[k, dy], parts[dy], sems.at[dy - 1]))
        waits[dy][0].start()
    return waits


def hidden_conv_kernel(
    c_in, stats, gain, shift, w_first, w_second, cw, c_ref, st, *rest, k, lo, n_in, strip, total, axis
):
    *w_next, a3, wbuf, sems = rest
    refill = None
    if w_next:
        (w_first,) = w_next
        refill = pltpu.make_async_copy(cw.at[k + 2, 0], w_first, sems.at[2])
    w_parts = [w_first, w_second, wbuf.at[0]]
    waits = weight_copies(cw, k + 1, w_parts, 2, sems)
    mean, scale, bias = norm_terms(stats, gain, shift, k, total)

    def row_at(i):
        x = jnp.maximum((c_in[i] - mean) * scale + bias, 0.0)
        return masked(x, inside(lo + i, strip, axis))

    write_stats(
        st, *run_conv(row_at, n_in, a3, w_parts, waits, c_ref, 0, lo + 1, strip, tile=SHAPES[k], refill=refill and (refill,))
    )
    if refill is not None:
        refill.wait()


def joined_conv_kernel(
    c_in, stats, gain, shift, w_in, feature, cw, c_ref, st, w_first, w_second, joined, a3, wbuf, sems,
    *, k, lo, n_in, strip, total, axis
):
    w_parts = [w_first, wbuf.at[0], wbuf.at[1]]
    waits = weight_copies(cw, k + 1, w_parts, 1, sems)
    late = pltpu.make_async_copy(cw.at[k + 2, 1], w_second, sems.at[3])
    refill = pltpu.make_async_copy(cw.at[k + 2, 0], w_first, sems.at[2])
    mean, scale, bias = norm_terms(stats, gain, shift, k, total)

    def row_at(i):
        y = (feature[i].astype(F32) + ((c_in[i] - mean) * scale + bias)).astype(BF)
        joined[i] = y
        return masked(relu_row(y), inside(lo + i, strip, axis))

    write_stats(
        st, *run_conv(row_at, n_in, a3, w_parts, waits, c_ref, 0, lo + 1, strip, tile=SHAPES[k], refill=(refill, late))
    )
    late.wait()
    refill.wait()


def final_kernel(joined, c_in, stats, gain, shift, out, rows, sems, *, k, total):
    mean, scale, bias = norm_terms(stats, gain, shift, k, total)
    copies = []
    for i in range(0, rows.shape[0], 2):
        for j in (i, i + 1):
            rows[j] = (joined[j + 2].astype(F32) + ((c_in[j] - mean) * scale + bias)).astype(BF)
        copies.append(pltpu.make_async_copy(rows.at[i : i + 2], out.at[i : i + 2], sems.at[i // 2]))
        copies[-1].start()
    for c in copies:
        c.wait()


def sent_to_all(value, axis):
    return lax.all_to_all(value, axis, 0, 0, tiled=True)


def reduce_all(partial):
    near = sent_to_all(partial, "row").sum(axis=0)
    far = lax.axis_size("img")
    return sent_to_all(jnp.broadcast_to(near[None], (far, *near.shape)), "img")


def swapped(value, firsts):
    pairs = [(i, (i + 1) % lax.axis_size("row")) for i in firsts]
    return lax.ppermute(value, "row", pairs + [(j, i) for i, j in pairs])


def on_device(tokens, proj_weight, proj_bias, conv_weight, bn_gain, bn_bias):
    imgs, strip, cols, embed = tokens.shape
    ch = proj_weight.shape[1]
    nrow = lax.axis_size("row")
    total = float(lax.axis_size("img") * nrow * imgs * strip * cols)
    weights = in_hbm(conv_weight)
    norm_args = (bn_gain, bn_bias)

    half = sds((HALO, cols, ch), BF)
    w_third = sds((3, ch, ch), BF)
    token_rows = in_hbm(tokens[0])
    far, pw, pb = pl.pallas_call(
        functools.partial(far_proj_kernel, axis="row"),
        out_shape=(half, sds((embed, ch), BF), sds((1, ch), F32)),
        in_specs=[HBM] * 3,
        out_specs=(VM,) * 3,
        scratch_shapes=[pltpu.VMEM((HALO, cols, embed), BF), pltpu.SemaphoreType.DMA((3,))],
        compiler_params=PARAMS,
    )(token_rows, in_hbm(proj_weight), in_hbm(proj_bias[None]))
    got_far = swapped(far, range(1, nrow, 2))
    near_call = pl.pallas_call(
        functools.partial(near_proj_kernel, axis="row"),
        out_shape=half,
        in_specs=[VM, VM, HBM],
        out_specs=VM,
        scratch_shapes=[pltpu.VMEM((HALO, cols, embed), BF), pltpu.SemaphoreType.DMA(())],
        compiler_params=PARAMS,
        cost_estimate=pl.CostEstimate(
            flops=2 * embed * ch * cols * HALO, transcendentals=0, bytes_accessed=2 * HALO * cols * embed
        ),
    )
    near = near_call(in_vmem(pw), in_vmem(pb), token_rows)
    got_near = swapped(near, range(0, nrow - 1, 2))
    far, near, got_far, got_near = map(in_vmem, (far, near, got_far, got_near))

    field = sds((strip + 2 * HALO - 2, cols, ch), F32)
    stat = sds((nrow, 1, 2 * ch), F32)
    context = sds((strip + 4, cols, ch), BF)

    def rows_scratch(rows):
        return pltpu.VMEM((rows, cols, 3 * ch), BF)

    sums = sds((2, 8, ch), F32)

    def conv_flops(rows):
        return pl.CostEstimate(
            flops=2 * 9 * ch * ch * cols * rows, transcendentals=0, bytes_accessed=9 * ch * ch * 2
        )

    c, part, w0, w_first, w_second = pl.pallas_call(
        functools.partial(conv0_inner_kernel, strip=strip, axis="row"),
        out_shape=(field, sums, sds((3, 3, ch, ch), BF), w_third, w_third),
        in_specs=[VM, VM, HBM],
        out_specs=(VM,) * 5,
        scratch_shapes=[rows_scratch(strip), pltpu.SemaphoreType.DMA((5,))],
        compiler_params=PARAMS,
        cost_estimate=conv_flops(strip - 2),
    )(far, near, weights)
    w0 = in_vmem(w0)
    c, part, feature = pl.pallas_call(
        functools.partial(conv0_near_kernel, strip=strip, axis="row"),
        out_shape=(field, sums, context),
        in_specs=[VM] * 6,
        out_specs=(VM,) * 3,
        input_output_aliases={5: 0},
        scratch_shapes=[rows_scratch(HALO + 2)],
        compiler_params=PARAMS,
        cost_estimate=conv_flops(HALO),
    )(got_near, far, near, w0, in_vmem(part), in_vmem(c))
    c, st, feature = pl.pallas_call(
        functools.partial(conv0_far_kernel, strip=strip, axis="row"),
        out_shape=(field, stat, context),
        in_specs=[VM] * 6,
        out_specs=(VM,) * 3,
        input_output_aliases={4: 0, 5: 2},
        scratch_shapes=[rows_scratch(HALO + 2)],
        compiler_params=PARAMS,
        cost_estimate=conv_flops(HALO),
    )(got_far, far, w0, in_vmem(part), in_vmem(c), in_vmem(feature))

    def call(kernel, extra_in, extra_out, n_in, aliases, **kw):
        args = (in_vmem(c), in_vmem(st), *norm_args, *map(in_vmem, extra_in))
        return pl.pallas_call(
            functools.partial(kernel, n_in=n_in, strip=strip, total=total, axis="row", **kw),
            out_shape=(field, stat, *extra_out),
            in_specs=[VM] * len(args) + [HBM],
            out_specs=(VM,) * (2 + len(extra_out)),
            input_output_aliases={0: 0, **aliases},
            scratch_shapes=[
                rows_scratch(n_in),
                pltpu.VMEM((2, 3, ch, ch), BF),
                pltpu.SemaphoreType.DMA((4,)),
            ],
            compiler_params=PARAMS,
        )(*args, weights)

    st = reduce_all(st)
    c, st, w_first = call(
        hidden_conv_kernel, (w_first, w_second), (w_third,), strip + 6, {4: 2}, k=0, lo=-3
    )
    st = reduce_all(st)
    c, st, w_first, w_second, joined = call(
        joined_conv_kernel, (w_first, feature), (w_third, w_third, context), strip + 4, {4: 2, 5: 4}, k=1, lo=-2
    )
    st = reduce_all(st)
    c, st = call(hidden_conv_kernel, (w_first, w_second), (), strip + 2, {}, k=2, lo=-1)
    st = reduce_all(st)
    out = pl.pallas_call(
        functools.partial(final_kernel, k=3, total=total),
        out_shape=sds((strip, cols, ch), BF),
        in_specs=[VM] * 5,
        out_specs=HBM,
        scratch_shapes=[pltpu.VMEM((strip, cols, ch), BF), pltpu.SemaphoreType.DMA((strip // 2,))],
        compiler_params=PARAMS,
    )(in_vmem(joined), in_vmem(c), in_vmem(st), *norm_args)
    return out[None]


def solution(mesh):
    placed = (P("img", "row", None, None), P(), P(), P(), P(), P())
    return jax.shard_map(
        on_device, mesh=mesh, in_specs=placed, out_specs=P("img", "row", None, None), check_vma=False
    )
```
